512 devices in a mesh: contract: 32 (over z, y_lo), out: 16 (over y_hi, x, core).
Axes of the slice: x: 4, y: 4 (y_hi: 2, y_lo: 2; y = y_hi * 2 + y_lo), z: 16, core: 2. Of those that a mesh axis runs over, the one named last changes fastest.
Arguments:
- chol: bfloat16 [128, 1024, 640], P('out', 'contract'), may hold values from -1.1953125 to 1.1953125
- amplitudes: bfloat16 [128, 32768], P('out', 'contract'), may hold values from -0.0625 to 0.0625
- tile_pairs: int32 [64, 2], replicated, may hold values from 0 to 7, as said below
- partner: int32 [64], replicated, may hold values from 0 to 63, as said below
- pair_swap: int32 [128], replicated, may hold values from 0 to 127, as said below
Outputs:
- residual: float32 [64, 128, 256], P('out', 'contract')
The draws below stay inside these ranges and needn't reach their ends.
Inputs may be any that keep to these rules, and one draw needn't show every extreme that they name: `tile_pairs`: each ordered pair of tiles of 0 to 7 stands at exactly one slot. partner[s] is the slot holding the pair of slot s reversed; a diagonal pair is its own partner. `pair_swap`: an involution without fixed points that maps each aligned block of 4 pairs into itself.
All inputs are finite; a program needn't handle non-finite values.
Results may differ from the reference program's by a relative error of at most 0.0029.
Values may be sent and summed in bfloat16 or wider, within the bound.
No kernel may reach another device: no remote copies, remote signals or barrier semaphores. Data moves between devices by JAX's collectives and lax.ppermute only.
A program may use at most 128 MiB of HBM per device.

```python
import jax
import jax.numpy as jnp
from jax import lax

V = 1024
P_SIZE = 640
TS = 16
NTILE = 8
DW = 32
OCC_DEV = 4
NO = 128
VW = 128
NT = 64


def tile_order(key):
    return jax.random.permutation(jax.random.fold_in(key, 11), NTILE * NTILE).astype(jnp.int32)


def draw_tile_pairs(key, part):
    order = tile_order(key)
    return jnp.stack([order // NTILE, order % NTILE], axis=1).astype(jnp.int32)


def draw_partner(key, part):
    order = tile_order(key)
    where = jnp.argsort(order, stable=True).astype(jnp.int32)
    swapped = order % NTILE * NTILE + order // NTILE
    return where[swapped].astype(jnp.int32)


def draw_pair_swap(key, part):
    keys = jax.random.split(jax.random.fold_in(key, 23), NO // OCC_DEV)

    def one_block(subkey):
        order = jax.random.permutation(subkey, OCC_DEV).astype(jnp.int32)
        evens = order[0::2]
        odds = order[1::2]
        result = jnp.zeros((OCC_DEV,), jnp.int32).at[evens].set(odds)
        return result.at[odds].set(evens)
    local = jax.vmap(one_block)(keys)
    base = (jnp.arange(NO // OCC_DEV, dtype=jnp.int32) * OCC_DEV)[:, None]
    return (local + base).reshape(NO).astype(jnp.int32)


def raised(drawn, rng, source, target, shards_of, factor):
    def block_of(dim):
        return (jnp.arange(drawn.shape[dim]) // (drawn.shape[dim] // shards_of)).reshape((-1,) + (1,) * (drawn.ndim - 1 - dim))

    first = jax.random.permutation(rng, shards_of)[block_of(target)]
    other_side = (block_of(target) + shards_of // 2) % shards_of
    return jnp.where((block_of(source) == first) | (block_of(source) == other_side), factor * drawn, drawn)


def block_levels(key, dims, pieces, least, largest):
    factor_of, own = 1.0, jax.random.fold_in(key, 6)
    for dim, blocks in pieces:
        steps = jnp.exp(jax.random.uniform(jax.random.fold_in(own, dim), (blocks,), jnp.float32, least / len(pieces), largest / len(pieces)))
        factor_of = factor_of * jnp.repeat(steps, dims[dim] // blocks).reshape([-1 if axis == dim else 1 for axis in range(len(dims))])
    return factor_of


def normal_values(stream_key, extent, width, bound, cuts=(), held_as=jnp.bfloat16):
    gain = block_levels(stream_key, extent, cuts, -0.22, 0.18) if cuts else 1.0
    entries = jax.random.normal(stream_key, extent, jnp.float32) * width * gain
    return jnp.minimum(jnp.maximum(entries, -bound), bound).astype(held_as)


def heavy_noise(own_key, extent, width, most, pieces, heavy, kind=jnp.bfloat16):
    values = width * jax.random.normal(own_key, extent, jnp.float32)
    if pieces:
        values = values * block_levels(own_key, extent, pieces, -0.22, 0.18)
    return jnp.clip(raised(values, jax.random.fold_in(own_key, 3), *heavy), -most, most).astype(kind)


def setup_inputs(seed: int = 0) -> dict:
    key_list = jax.random.split(jax.random.key(seed), 6)
    return {
        "chol": normal_values(key_list[0], (VW, V, P_SIZE), 0.2, 1.1953125, ((0, 16), (1, 32))),
        "amplitudes": heavy_noise(key_list[1], (NO, V * DW), (V * DW) ** -0.5, 0.0625, ((0, 16), (1, 32)), (1, 0, 32, 2.75)),
        "tile_pairs": draw_tile_pairs(jax.random.fold_in(key_list[5], 71), 0),
        "partner": draw_partner(jax.random.fold_in(key_list[5], 71), 0),
        "pair_swap": draw_pair_swap(jax.random.fold_in(key_list[5], 71), 0),
    }


def reference(chol, amplitudes, tile_pairs, partner, pair_swap):
    window = chol[:, :DW, :]
    amps = amplitudes.reshape(NO, V, DW).astype(jnp.float32)

    def one_slot(pair):
        left = lax.dynamic_slice_in_dim(chol, (pair[0] * TS).astype(jnp.int32), TS, 0)
        right = lax.dynamic_slice_in_dim(window, (pair[1] * TS).astype(jnp.int32), TS, 0)
        integral = jnp.einsum('acp,bdp->abcd', left.astype(jnp.float32), right.astype(jnp.float32), precision=lax.Precision.HIGHEST).astype(jnp.bfloat16)
        return jnp.einsum('icd,abcd->iab', amps, integral.astype(jnp.float32), precision=lax.Precision.HIGHEST)

    ladder = lax.map(one_slot, tile_pairs)
    mirror = jnp.take(jnp.take(ladder, partner, axis=0), pair_swap, axis=1)
    mirror = jnp.transpose(mirror, (0, 1, 3, 2))
    return (ladder + mirror).reshape(NT, NO, TS * TS)
```

```python
import functools

import jax
import jax.numpy as jnp
from jax import lax
from jax.experimental import pallas as pl
from jax.experimental.pallas import tpu as pltpu
from jax.sharding import Mesh
from jax.sharding import PartitionSpec as P

TS = 16
LANES = 128
CONTRACT = ("z", "yl")
OUT = ("yh", "x", "core")
PAIR = [(0, 1), (1, 0)]


def exchange(array, axes):
    return lax.all_to_all(array, axes, 0, 0, tiled=True)


def sent_to_all(array, axes):
    count = lax.axis_size(axes)
    return exchange(jnp.broadcast_to(array[None], (count, *array.shape)), axes)


def ladder_kernel(
    place_ref, near_ref, far_ref, amps_ref, amps_far_ref, own_ref, opposite_ref, out_ref, stack_ref
):
    core, x_here, yh = place_ref[0], place_ref[1], place_ref[2]
    _, ring, pair_rows, _ = near_ref.shape
    c_pairs = near_ref.shape[0] - 1
    a_dev = pair_rows // 2
    b_count, depth, _ = stack_ref.shape
    b_dev = b_count // 2
    d_count = own_ref.shape[0] // b_dev
    order = [lax.rem(x_here + ring - x, ring) for x in range(ring)]
    right = jnp.concatenate([own_ref[...], opposite_ref[...]], axis=0)
    for n in range(0, c_pairs, 2):
        left = jnp.concatenate(
            [ref[m, order[x]] for m in (n, n + 1) for ref in (near_ref, far_ref) for x in range(ring)],
            axis=0,
        )
        part = lax.dot_general(
            right, left, (((1,), (1,)), ((), ())), preferred_element_type=jnp.float32
        ).astype(jnp.bfloat16)
        part = part.reshape(b_count, d_count, 2 * LANES)
        for h in range(2):
            rows = (n + h) * d_count
            stack_ref[:, rows : rows + d_count, :] = part[:, :, h * LANES : (h + 1) * LANES]
    amps = jnp.concatenate(
        [amps_ref[q, :, :depth] for q in range(amps_ref.shape[0])]
        + [amps_far_ref[q, :, :depth] for q in range(amps_far_ref.shape[0])],
        axis=0,
    )
    blocks = amps.shape[0] // pair_rows
    odd = lax.rem(lax.broadcasted_iota(jnp.int32, (1, 1, LANES), 2) // a_dev, 2) == 1
    for q in range(b_count // 2):
        sums = []
        for b, step in ((2 * q, LANES - a_dev), (2 * q + 1, a_dev)):
            full = jnp.dot(amps, stack_ref[b], preferred_element_type=jnp.float32)
            full = full.reshape(blocks, 2, a_dev, LANES)
            mixed = jnp.where(odd, full[:, 1], full[:, 0]).reshape(blocks * a_dev, LANES)
            sums.append(mixed + pltpu.roll(mixed, step, 1))
        found = jnp.where(odd[0], sums[1], sums[0])
        found = pltpu.roll(found, core * (LANES // 2), 1)
        half = lax.rem(yh + q // (b_count // 4), 2)
        column = pl.multiple_of((half * (b_count // 4) + q % (b_count // 4)) * LANES, LANES)
        for block in range(blocks):
            other_yh, other_core, shift = block // (2 * ring), block // ring % 2, block % ring
            source = lax.rem(x_here + ring - shift, ring)
            place = (lax.rem(yh + other_yh, 2) * ring + source) * 2 + lax.rem(core + other_core, 2)
            for h in range(2):
                rows = found[block * a_dev + h * (a_dev // 2) : block * a_dev + (h + 1) * (a_dev // 2)]
                out_ref[2 * place + h, :, pl.ds(column, LANES)] = rows


def ladder_partials(place, near, far, amps, amps_far, own, opposite, i_count, con_count):
    b_count = 2 * near.shape[2] // 2
    d_count = own.shape[0] // (b_count // 2)
    depth = (near.shape[0] - 1) * d_count
    pairs = 2 * near.size * (2 * own.shape[0])
    return pl.pallas_call(
        ladder_kernel,
        out_shape=jax.ShapeDtypeStruct(
            (con_count, i_count // con_count, b_count * LANES // 2), jnp.float32
        ),
        in_specs=[pl.BlockSpec(memory_space=pltpu.SMEM)]
        + [pl.BlockSpec(memory_space=pltpu.VMEM)] * 6,
        out_specs=pl.BlockSpec(memory_space=pltpu.VMEM),
        scratch_shapes=[pltpu.VMEM((b_count, depth, LANES), jnp.bfloat16)],
        compiler_params=pltpu.CompilerParams(vmem_limit_bytes=20 * 1024 * 1024),
        cost_estimate=pl.CostEstimate(
            flops=2 * pairs, bytes_accessed=4 * near.size, transcendentals=0
        ),
    )(place, near, far, amps, amps_far, own, opposite)


def on_device(chol, amplitudes, tile_pairs, partner, pair_swap):
    out_count = lax.axis_size(OUT)
    con_count = lax.axis_size(CONTRACT)
    ring = lax.axis_size("x")
    a_dev, c_dev, p_size = chol.shape
    i_dev = amplitudes.shape[0]
    i_count = i_dev * out_count
    half = c_dev // 2
    pair_rows = 2 * a_dev

    with jax.named_scope("pack"):
        rows = jnp.transpose(chol.reshape(a_dev, 2, half, p_size), (2, 1, 0, 3))
        extra = jnp.transpose(amplitudes.reshape(i_dev, 2, -1), (1, 0, 2)).reshape(1, pair_rows, -1)
        extra = jnp.pad(extra, ((0, 0), (0, 0), (0, p_size - extra.shape[2])))
        packed = jnp.concatenate([rows.reshape(half, pair_rows, p_size), extra], axis=0)
    with jax.named_scope("ring"):
        near = [packed] + [
            lax.ppermute(packed, "x", [(x, (x + shift) % ring) for x in range(ring)])
            for shift in range(1, ring)
        ]
        near = jnp.stack(near, axis=1)

    with jax.named_scope("scatter"):
        slices = exchange(chol.reshape(con_count, -1, p_size), CONTRACT)
    with jax.named_scope("spread"):
        own = sent_to_all(slices[0], CONTRACT).reshape(a_dev * c_dev, p_size)

    with jax.named_scope("cores"):
        far = lax.ppermute(near, "core", PAIR)
    with jax.named_scope("amps"):
        amps = jnp.concatenate([near[half], far[half]], axis=0)
        amps_far = lax.ppermute(amps, "yh", PAIR)
    with jax.named_scope("window"):
        opposite = lax.ppermute(own, "yh", PAIR)

    place = jnp.stack([lax.axis_index("core"), lax.axis_index("x"), lax.axis_index("yh")])
    partial = ladder_partials(
        place, near, far, amps, amps_far, own, opposite, i_count, con_count
    )
    ladder = jnp.sum(exchange(partial, CONTRACT), axis=0)

    occ_dev = i_count // con_count
    ladder = ladder.reshape(occ_dev, 2, a_dev // 2, 2, ring, 2, a_dev)
    ladder = jnp.transpose(ladder, (4, 1, 0, 3, 6, 2, 5)).reshape(2 * ring, occ_dev, TS * a_dev)
    every = sent_to_all(ladder, OUT).reshape(-1, occ_dev, TS * a_dev)

    slot_count = tile_pairs.shape[0] // out_count
    first = lax.axis_index(OUT) * slot_count
    pairs = lax.dynamic_slice_in_dim(tile_pairs, first, slot_count, 0)

    def whole_tiles(a_tile, b_tile):
        holder = (a_tile // ring * ring + b_tile % ring) * 2
        inner = a_tile % ring * 2 + b_tile // ring
        spots = (holder[:, None] + jnp.arange(2)) * (2 * ring) + inner[:, None]
        found = jnp.take(every, spots.reshape(-1), axis=0, mode="clip")
        return found.reshape(slot_count, 2, occ_dev, TS, a_dev)

    own_swap = lax.dynamic_slice_in_dim(
        pair_swap, lax.axis_index(CONTRACT) * occ_dev, occ_dev, 0
    ) - lax.axis_index(CONTRACT) * occ_dev
    straight = jnp.transpose(whole_tiles(pairs[:, 0], pairs[:, 1]), (0, 2, 3, 1, 4))
    mirror = whole_tiles(pairs[:, 1], pairs[:, 0])
    mirror = jnp.take(mirror, own_swap, axis=2, mode="clip")
    mirror = jnp.transpose(mirror, (0, 2, 1, 4, 3))
    residual = straight.reshape(slot_count, occ_dev, TS, TS) + mirror.reshape(
        slot_count, occ_dev, TS, TS
    )
    return residual.reshape(slot_count, occ_dev, TS * TS)


def solution(mesh):
    torus = Mesh(mesh.devices.reshape(16, 2, 2, 4, 2), ("z", "yl", "yh", "x", "core"))
    in_specs = (P(OUT, CONTRACT, None), P(OUT, CONTRACT), P(), P(), P())
    out_specs = P(OUT, CONTRACT, None)
    return jax.shard_map(
        on_device, mesh=torus, in_specs=in_specs, out_specs=out_specs, check_vma=False
    )
```

```python
import jax
import jax.numpy as jnp
from jax import lax
from jax.experimental import pallas as pl
from jax.experimental.pallas import tpu as pltpu
from jax.sharding import Mesh
from jax.sharding import PartitionSpec as P

TS = 16
LANES = 128
CONTRACT = ("z", "yl")
OUT = ("yh", "x", "core")
PAIR = [(0, 1), (1, 0)]


def exchange(array, axes):
    return lax.all_to_all(array, axes, 0, 0, tiled=True)


def sent_to_all(array, axes):
    count = lax.axis_size(axes)
    return exchange(jnp.broadcast_to(array[None], (count, *array.shape)), axes)


def ladder_kernel(
    place_ref, near_ref, far_ref, amps_ref, amps_far_ref, right_ref, out_ref, stack_ref
):
    core, yh = place_ref[0], place_ref[1]
    b_count, depth, _ = stack_ref.shape
    ring, pair_rows = near_ref.shape[0], amps_ref.shape[1]
    c_pairs = near_ref.shape[1] // pair_rows - 1
    a_dev = pair_rows // 2
    d_count = right_ref.shape[0] // b_count
    right = right_ref[...]
    for n in range(0, c_pairs, 2):
        left = jnp.concatenate(
            [
                ref[x, m * pair_rows : (m + 1) * pair_rows, :]
                for m in (n, n + 1)
                for ref in (near_ref, far_ref)
                for x in range(ring)
            ],
            axis=0,
        )
        part = lax.dot_general(
            right, left, (((1,), (1,)), ((), ())), preferred_element_type=jnp.float32
        ).astype(jnp.bfloat16)
        part = part.reshape(b_count, d_count, 2 * LANES)
        for h in range(2):
            rows = (n + h) * d_count
            stack_ref[:, rows : rows + d_count, :] = part[:, :, h * LANES : (h + 1) * LANES]
    amps = jnp.concatenate(
        [amps_ref[q, :, :depth] for q in range(amps_ref.shape[0])]
        + [amps_far_ref[q, :, :depth] for q in range(amps_far_ref.shape[0])],
        axis=0,
    )
    blocks = amps.shape[0] // pair_rows
    odd = lax.rem(lax.broadcasted_iota(jnp.int32, (1, 1, LANES), 2) // a_dev, 2) == 1
    for q in range(b_count // 2):
        sums = []
        for b, step in ((2 * q, LANES - a_dev), (2 * q + 1, a_dev)):
            full = jnp.dot(amps, stack_ref[b], preferred_element_type=jnp.float32)
            full = full.reshape(blocks, 2, a_dev, LANES)
            mixed = jnp.where(odd, full[:, 1], full[:, 0]).reshape(blocks * a_dev, LANES)
            sums.append(mixed + pltpu.roll(mixed, step, 1))
        found = jnp.where(odd[0], sums[1], sums[0])
        found = pltpu.roll(found, core * (LANES // 2), 1)
        found = found.astype(out_ref.dtype)
        for block in range(blocks):
            other_yh, other_core, x = block // (2 * ring), block // ring % 2, block % ring
            place = (lax.rem(yh + other_yh, 2) * ring + x) * 2 + lax.rem(core + other_core, 2)
            for h in range(2):
                rows = found[block * a_dev + h * (a_dev // 2) : block * a_dev + (h + 1) * (a_dev // 2)]
                out_ref[2 * place + h, :, q * LANES : (q + 1) * LANES] = rows


def ladder_partials(place, near, far, amps, amps_far, right, i_count, con_count):
    b_count = amps.shape[1]
    depth = (near.shape[1] // b_count - 1) * (right.shape[0] // b_count)
    pairs = 2 * near.size * right.shape[0]
    return pl.pallas_call(
        ladder_kernel,
        out_shape=jax.ShapeDtypeStruct(
            (con_count, i_count // con_count, b_count * LANES // 2), jnp.bfloat16
        ),
        in_specs=[pl.BlockSpec(memory_space=pltpu.SMEM)]
        + [pl.BlockSpec(memory_space=pltpu.VMEM)] * 5,
        out_specs=pl.BlockSpec(memory_space=pltpu.VMEM),
        scratch_shapes=[pltpu.VMEM((b_count, depth, LANES), jnp.bfloat16)],
        compiler_params=pltpu.CompilerParams(vmem_limit_bytes=12 * 1024 * 1024),
        cost_estimate=pl.CostEstimate(
            flops=2 * pairs, bytes_accessed=4 * near.size, transcendentals=0
        ),
    )(place, near, far, amps, amps_far, right)


def on_device(chol, amplitudes, tile_pairs, partner, pair_swap):
    out_count = lax.axis_size(OUT)
    con_count = lax.axis_size(CONTRACT)
    ring = lax.axis_size("x")
    a_dev, c_dev, p_size = chol.shape
    i_dev = amplitudes.shape[0]
    i_count = i_dev * out_count
    half = c_dev // 2
    pair_rows = 2 * a_dev

    rows = jnp.transpose(chol.reshape(a_dev, 2, half, p_size), (2, 1, 0, 3))
    extra = jnp.transpose(amplitudes.reshape(i_dev, 2, -1), (1, 0, 2)).reshape(1, pair_rows, -1)
    extra = jnp.pad(extra, ((0, 0), (0, 0), (0, p_size - extra.shape[2])))
    packed = jnp.concatenate([rows.reshape(half, pair_rows, p_size), extra], axis=0)
    near = sent_to_all(packed.reshape(-1, p_size), "x")

    z, yl = lax.axis_index("z"), lax.axis_index("yl")
    depth_z = lax.axis_size("z")
    window = chol.reshape(2, -1, p_size)
    piece = jnp.where(yl == 0, window[0], lax.ppermute(window[1], CONTRACT, [(0, 1)]))
    got = sum(lax.ppermute(piece, "z", [(0, to)]) for to in (8, 12, 4))
    piece = jnp.where(z == 0, piece, got)
    got = sum(
        lax.ppermute(
            piece, "z", [(at, (at + step) % depth_z) for at in range(0, depth_z, 4)]
        )
        for step in (2, 1, -1)
    )
    piece = jnp.where(z % 4 == 0, piece, got)
    right = sent_to_all(piece, ("yh", "yl")).reshape(-1, p_size)

    far = lax.ppermute(near, "core", PAIR)
    amps = jnp.concatenate([near[:, -pair_rows:], far[:, -pair_rows:]], axis=0)
    amps_far = lax.ppermute(amps, "yh", PAIR)

    place = jnp.stack([lax.axis_index("core"), lax.axis_index("yh")])
    partial = ladder_partials(place, near, far, amps, amps_far, right, i_count, con_count)
    ladder = jnp.sum(exchange(partial, CONTRACT).astype(jnp.float32), axis=0)

    occ_dev = i_count // con_count
    ladder = ladder.reshape(occ_dev, 2, a_dev // 2, 2, ring, 2, a_dev)
    ladder = jnp.transpose(ladder, (4, 1, 0, 3, 6, 2, 5)).reshape(2 * ring, occ_dev, TS * a_dev)
    every = sent_to_all(ladder, OUT).reshape(-1, occ_dev, TS * a_dev)

    slot_count = tile_pairs.shape[0] // out_count
    first = lax.axis_index(OUT) * slot_count
    pairs = lax.dynamic_slice_in_dim(tile_pairs, first, slot_count, 0)

    def whole_tiles(a_tile, b_tile):
        holder = (a_tile // ring * ring + b_tile % ring) * 2
        inner = a_tile % ring * 2 + b_tile // ring
        spots = (holder[:, None] + jnp.arange(2)) * (2 * ring) + inner[:, None]
        found = jnp.take(every, spots.reshape(-1), axis=0, mode="clip")
        return found.reshape(slot_count, 2, occ_dev, TS, a_dev)

    own_swap = lax.dynamic_slice_in_dim(
        pair_swap, lax.axis_index(CONTRACT) * occ_dev, occ_dev, 0
    ) - lax.axis_index(CONTRACT) * occ_dev
    straight = jnp.transpose(whole_tiles(pairs[:, 0], pairs[:, 1]), (0, 2, 3, 1, 4))
    mirror = whole_tiles(pairs[:, 1], pairs[:, 0])
    mirror = jnp.take(mirror, own_swap, axis=2, mode="clip")
    mirror = jnp.transpose(mirror, (0, 2, 1, 4, 3))
    residual = straight.reshape(slot_count, occ_dev, TS, TS) + mirror.reshape(
        slot_count, occ_dev, TS, TS
    )
    return residual.reshape(slot_count, occ_dev, TS * TS)


def solution(mesh):
    torus = Mesh(mesh.devices.reshape(16, 2, 2, 4, 2), ("z", "yl", "yh", "x", "core"))
    in_specs = (P(OUT, CONTRACT, None), P(OUT, CONTRACT), P(), P(), P())
    out_specs = P(OUT, CONTRACT, None)

    return jax.shard_map(
        on_device, mesh=torus, in_specs=in_specs, out_specs=out_specs, check_vma=False
    )
```

```python
import functools

import jax
import jax.numpy as jnp
from jax import lax
from jax.experimental import pallas as pl
from jax.experimental.pallas import tpu as pltpu
from jax.sharding import Mesh
from jax.sharding import PartitionSpec as P

TS = 16
LANES = 128
CONTRACT = ("z", "yl")
OUT = ("yh", "x", "core")
PAIR = [(0, 1), (1, 0)]


def exchange(array, axes):
    return lax.all_to_all(array, axes, 0, 0, tiled=True)


def sent_to_all(array, axes):
    count = lax.axis_size(axes)
    return exchange(jnp.broadcast_to(array[None], (count, *array.shape)), axes)


def ladder_kernel(place_ref, near_ref, far_ref, right_ref, out_ref, stack_ref):
    core, yh = place_ref[0], place_ref[1]
    b_count, depth, _ = stack_ref.shape
    ring, pair_rows = near_ref.shape[0], b_count
    c_pairs = near_ref.shape[1] // pair_rows - 2
    a_dev = pair_rows // 2
    d_count = right_ref.shape[0] // b_count
    right = right_ref[...]
    for n in range(0, c_pairs, 2):
        left = jnp.concatenate(
            [
                ref[x, m * pair_rows : (m + 1) * pair_rows, :]
                for m in (n, n + 1)
                for x in range(ring)
                for ref in (near_ref, far_ref)
            ],
            axis=0,
        )
        part = lax.dot_general(
            right, left, (((1,), (1,)), ((), ())), preferred_element_type=jnp.float32
        ).astype(jnp.bfloat16)
        part = part.reshape(b_count, d_count, 2 * LANES)
        for h in range(2):
            rows = (n + h) * d_count
            stack_ref[:, rows : rows + d_count, :] = part[:, :, h * LANES : (h + 1) * LANES]
    amps = jnp.concatenate(
        [
            ref[x, m * pair_rows : (m + 1) * pair_rows, :depth]
            for m in (c_pairs, c_pairs + 1)
            for ref in (near_ref, far_ref)
            for x in range(ring)
        ],
        axis=0,
    )
    blocks = 4 * ring
    odd = lax.rem(lax.broadcasted_iota(jnp.int32, (1, 1, LANES), 2) // a_dev, 2) == 1
    for q in range(b_count // 2):
        sums = []
        for b, step in ((2 * q, LANES - a_dev), (2 * q + 1, a_dev)):
            full = jnp.dot(amps, stack_ref[b], preferred_element_type=jnp.float32)
            full = full.reshape(blocks, 2, a_dev, LANES)
            mixed = jnp.where(odd, full[:, 1], full[:, 0]).reshape(blocks * a_dev, LANES)
            sums.append(mixed + pltpu.roll(mixed, step, 1))
        found = jnp.where(odd[0], sums[1], sums[0]).astype(out_ref.dtype)
        for block in range(blocks):
            other_yh, other_core, x = block // (2 * ring), block // ring % 2, block % ring
            place = (lax.rem(yh + other_yh, 2) * ring + x) * 2 + lax.rem(core + other_core, 2)
            for h in range(2):
                rows = found[block * a_dev + h * (a_dev // 2) : block * a_dev + (h + 1) * (a_dev // 2)]
                out_ref[2 * place + h, :, q * LANES : (q + 1) * LANES] = rows


def in_vmem(count):
    return [pl.BlockSpec(memory_space=pltpu.VMEM)] * count


def ladder_partials(place, near, far, right, b_count, i_count, con_count):
    depth = (near.shape[1] // b_count - 2) * (right.shape[0] // b_count)
    pairs = 2 * near.size * right.shape[0]
    return pl.pallas_call(
        ladder_kernel,
        out_shape=jax.ShapeDtypeStruct(
            (con_count, i_count // con_count, b_count * LANES // 2), jnp.bfloat16
        ),
        in_specs=[pl.BlockSpec(memory_space=pltpu.SMEM)] + in_vmem(3),
        out_specs=pl.BlockSpec(memory_space=pltpu.VMEM),
        scratch_shapes=[pltpu.VMEM((b_count, depth, LANES), jnp.bfloat16)],
        compiler_params=pltpu.CompilerParams(vmem_limit_bytes=12 * 1024 * 1024),
        cost_estimate=pl.CostEstimate(
            flops=2 * pairs, bytes_accessed=4 * near.size, transcendentals=0
        ),
    )(place, near, far, right)


def total_kernel(parts_ref, out_ref):
    total = parts_ref[0].astype(jnp.float32)
    for k in range(1, parts_ref.shape[0]):
        total = total + parts_ref[k].astype(jnp.float32)
    for o in range(out_ref.shape[0]):
        out_ref[o] = total


def totals(parts, copies):
    return pl.pallas_call(
        total_kernel,
        out_shape=jax.ShapeDtypeStruct((copies, *parts.shape[1:]), jnp.float32),
        in_specs=in_vmem(1),
        out_specs=pl.BlockSpec(memory_space=pltpu.VMEM),
        compiler_params=pltpu.CompilerParams(vmem_limit_bytes=4 * 1024 * 1024),
        cost_estimate=pl.CostEstimate(
            flops=parts.size, bytes_accessed=4 * parts.size, transcendentals=0
        ),
    )(parts)


def residual_kernel(ring, pairs_ref, swap_ref, every_ref, out_ref):
    slots, occ, width = out_ref.shape
    group = LANES // ring
    chunks = every_ref.shape[2] // LANES // 2
    lane_group = lax.broadcasted_iota(jnp.int32, (1, LANES), 1) // group

    def half_tile(a_tile, b_tile, c):
        holder = (a_tile // ring * ring + lax.rem(b_tile, ring)) * 2 + c
        first = b_tile // ring * (chunks * LANES)
        found = jnp.zeros((occ, LANES), jnp.float32)
        for m in range(chunks):
            block = every_ref[holder, :, pl.ds(pl.multiple_of(first + m * LANES, LANES), LANES)]
            shift = lax.rem((m + ring - lax.rem(a_tile, ring)) * group, LANES)
            found = jnp.where(lane_group == m, pltpu.roll(block, shift, 1), found)
        return found

    def tiles(role):
        return jnp.concatenate(
            [
                jnp.concatenate(
                    [half_tile(pairs_ref[s, role], pairs_ref[s, 1 - role], c) for c in range(2)],
                    axis=1,
                )
                for s in range(slots)
            ],
            axis=0,
        )

    def placed(rows, spot):
        column = lax.broadcasted_iota(jnp.int32, (width, width), 1)
        chosen = (column == spot).astype(jnp.float32)
        return jnp.dot(
            rows, chosen, preferred_element_type=jnp.float32, precision=lax.Precision.HIGHEST
        )

    lane = lax.broadcasted_iota(jnp.int32, (width, width), 0)
    core_b = lane // LANES
    core_a = lax.rem(lane // (group // 2) + core_b, 2)
    a = core_a * (TS // 2) + lax.rem(lane, TS // 2)
    b = core_b * (TS // 2) + lax.rem(lane, LANES) // group * 2 + lax.rem(lane // (TS // 2), 2)
    straight = placed(tiles(0), a * TS + b)
    mirror = placed(tiles(1), b * TS + a)
    row = lax.broadcasted_iota(jnp.int32, (slots * occ, slots * occ), 0)
    column = lax.broadcasted_iota(jnp.int32, (slots * occ, slots * occ), 1)
    source = row // occ * occ
    for i in range(occ):
        source = source + jnp.where(lax.rem(row, occ) == i, swap_ref[i], 0)
    turned = jnp.dot(
        (column == source).astype(jnp.float32),
        mirror,
        preferred_element_type=jnp.float32,
        precision=lax.Precision.HIGHEST,
    )
    total = straight + turned
    for s in range(slots):
        out_ref[s] = total[s * occ : (s + 1) * occ]


def residual_tiles(pairs, swap, every, ring):
    slots, occ = pairs.shape[0], swap.shape[0]
    return pl.pallas_call(
        functools.partial(residual_kernel, ring),
        out_shape=jax.ShapeDtypeStruct((slots, occ, TS * TS), jnp.float32),
        in_specs=[pl.BlockSpec(memory_space=pltpu.SMEM)] * 2 + in_vmem(1),
        out_specs=pl.BlockSpec(memory_space=pltpu.VMEM),
        compiler_params=pltpu.CompilerParams(vmem_limit_bytes=8 * 1024 * 1024),
        cost_estimate=pl.CostEstimate(
            flops=100 * every.size, bytes_accessed=4 * every.size, transcendentals=0
        ),
    )(pairs, swap, every)


def on_device(chol, amplitudes, tile_pairs, partner, pair_swap):
    out_count = lax.axis_size(OUT)
    con_count = lax.axis_size(CONTRACT)
    ring = lax.axis_size("x")
    a_dev, c_dev, p_size = chol.shape
    i_dev = amplitudes.shape[0]
    i_count = i_dev * out_count
    half = c_dev // 2
    pair_rows = 2 * a_dev

    other_amps = lax.ppermute(amplitudes, "yh", PAIR)
    rows = jnp.transpose(chol.reshape(a_dev, 2, half, p_size), (2, 1, 0, 3))
    extra = jnp.stack([amplitudes, other_amps], axis=0).reshape(2, i_dev, 2, -1)
    extra = jnp.transpose(extra, (0, 2, 1, 3)).reshape(2, pair_rows, -1)
    extra = jnp.pad(extra, ((0, 0), (0, 0), (0, p_size - extra.shape[2])))
    packed = jnp.concatenate([rows.reshape(half, pair_rows, p_size), extra], axis=0)
    near = sent_to_all(packed.reshape(-1, p_size), "x")

    z, yl = lax.axis_index("z"), lax.axis_index("yl")
    depth_z = lax.axis_size("z")
    window = chol.reshape(2, -1, p_size)
    piece = jnp.where(yl == 0, window[0], lax.ppermute(window[1], CONTRACT, [(0, 1)]))
    got = sum(lax.ppermute(piece, "z", [(0, to)]) for to in (8, 12, 4))
    piece = jnp.where(z == 0, piece, got)
    got = sum(
        lax.ppermute(
            piece, "z", [(at, (at + step) % depth_z) for at in range(0, depth_z, 4)]
        )
        for step in (2, 1, -1)
    )
    piece = jnp.where(z % 4 == 0, piece, got)
    right = sent_to_all(piece, ("yh", "yl")).reshape(-1, p_size)

    far = lax.ppermute(near, "core", PAIR)
    place = jnp.stack([lax.axis_index("core"), lax.axis_index("yh")])
    partial = ladder_partials(place, near, far, right, 2 * a_dev, i_count, con_count)
    every = exchange(totals(exchange(partial, CONTRACT), out_count), OUT)

    slot_count, occ_dev = tile_pairs.shape[0] // out_count, i_count // con_count
    first = lax.axis_index(OUT) * slot_count
    pairs = lax.dynamic_slice_in_dim(tile_pairs, first, slot_count, 0)
    first = lax.axis_index(CONTRACT) * occ_dev
    swap = lax.dynamic_slice_in_dim(pair_swap, first, occ_dev, 0) - first
    return residual_tiles(pairs, swap, every, ring)


def solution(mesh):
    torus = Mesh(mesh.devices.reshape(16, 2, 2, 4, 2), ("z", "yl", "yh", "x", "core"))
    in_specs = (P(OUT, CONTRACT, None), P(OUT, CONTRACT), P(), P(), P())
    out_specs = P(OUT, CONTRACT, None)

    return jax.shard_map(
        on_device, mesh=torus, in_specs=in_specs, out_specs=out_specs, check_vma=False
    )
```

```python
import functools

import jax
import jax.numpy as jnp
from jax import lax
from jax.experimental import pallas as pl
from jax.experimental.pallas import tpu as pltpu
from jax.sharding import Mesh
from jax.sharding import PartitionSpec as P

TS = 16
LANES = 128
CONTRACT = ("z", "yl")
OUT = ("yh", "x", "core")
PAIR = [(0, 1), (1, 0)]
RELAYS = (5, 11)


def exchange(array, axes):
    return lax.all_to_all(array, axes, 0, 0, tiled=True)


def sent_to_all(array, axes):
    count = lax.axis_size(axes)
    return exchange(jnp.broadcast_to(array[None], (count, *array.shape)), axes)


def ladder_kernel(place_ref, near_ref, far_ref, *refs):
    *quarter_refs, out_ref, stack_ref, right_ref = refs
    core, yh, own = place_ref[0], place_ref[1], place_ref[2]
    size = quarter_refs[0].shape[0]
    for q, ref in enumerate(quarter_refs):
        right_ref[pl.ds(pl.multiple_of((own ^ q) * size, size), size), :] = ref[...]
    b_count, depth, _ = stack_ref.shape
    ring, pair_rows = near_ref.shape[0], b_count
    c_pairs = near_ref.shape[1] // pair_rows - 2
    a_dev = pair_rows // 2
    d_count = right_ref.shape[0] // b_count
    right = right_ref[...]
    for n in range(0, c_pairs, 2):
        left = jnp.concatenate(
            [
                ref[x, m * pair_rows : (m + 1) * pair_rows, :]
                for m in (n, n + 1)
                for x in range(ring)
                for ref in (near_ref, far_ref)
            ],
            axis=0,
        )
        part = lax.dot_general(
            right, left, (((1,), (1,)), ((), ())), preferred_element_type=jnp.float32
        ).astype(jnp.bfloat16)
        part = part.reshape(b_count, d_count, 2 * LANES)
        for h in range(2):
            rows = (n + h) * d_count
            stack_ref[:, rows : rows + d_count, :] = part[:, :, h * LANES : (h + 1) * LANES]
    amps = jnp.concatenate(
        [
            ref[x, m * pair_rows : (m + 1) * pair_rows, :depth]
            for m in (c_pairs, c_pairs + 1)
            for ref in (near_ref, far_ref)
            for x in range(ring)
        ],
        axis=0,
    )
    blocks = 4 * ring
    odd = lax.rem(lax.broadcasted_iota(jnp.int32, (1, 1, LANES), 2) // a_dev, 2) == 1
    for q in range(b_count // 2):
        sums = []
        for b, step in ((2 * q, LANES - a_dev), (2 * q + 1, a_dev)):
            full = jnp.dot(amps, stack_ref[b], preferred_element_type=jnp.float32)
            full = full.reshape(blocks, 2, a_dev, LANES)
            mixed = jnp.where(odd, full[:, 1], full[:, 0]).reshape(blocks * a_dev, LANES)
            sums.append(mixed + pltpu.roll(mixed, step, 1))
        found = jnp.where(odd[0], sums[1], sums[0]).astype(out_ref.dtype)
        for block in range(blocks):
            other_yh, other_core, x = block // (2 * ring), block // ring % 2, block % ring
            place = (lax.rem(yh + other_yh, 2) * ring + x) * 2 + lax.rem(core + other_core, 2)
            for h in range(2):
                rows = found[block * a_dev + h * (a_dev // 2) : block * a_dev + (h + 1) * (a_dev // 2)]
                out_ref[2 * place + h, :, q * LANES : (q + 1) * LANES] = rows


def in_vmem(count):
    return [pl.BlockSpec(memory_space=pltpu.VMEM)] * count


def ladder_partials(place, near, far, quarters, b_count, i_count, con_count):
    right = (len(quarters) * quarters[0].shape[0], quarters[0].shape[1])
    depth = (near.shape[1] // b_count - 2) * (right[0] // b_count)
    pairs = 2 * near.size * right[0]
    return pl.pallas_call(
        ladder_kernel,
        out_shape=jax.ShapeDtypeStruct(
            (con_count, i_count // con_count, b_count * LANES // 2), jnp.bfloat16
        ),
        in_specs=[pl.BlockSpec(memory_space=pltpu.SMEM)] + in_vmem(2 + len(quarters)),
        out_specs=pl.BlockSpec(memory_space=pltpu.VMEM),
        scratch_shapes=[
            pltpu.VMEM((b_count, depth, LANES), jnp.bfloat16),
            pltpu.VMEM(right, jnp.bfloat16),
        ],
        compiler_params=pltpu.CompilerParams(vmem_limit_bytes=12 * 1024 * 1024),
        cost_estimate=pl.CostEstimate(
            flops=2 * pairs, bytes_accessed=4 * near.size, transcendentals=0
        ),
    )(place, near, far, *quarters)


def total_kernel(parts_ref, out_ref):
    total = parts_ref[0].astype(jnp.float32)
    for k in range(1, parts_ref.shape[0]):
        total = total + parts_ref[k].astype(jnp.float32)
    for o in range(out_ref.shape[0]):
        out_ref[o] = total


def totals(parts, copies):
    return pl.pallas_call(
        total_kernel,
        out_shape=jax.ShapeDtypeStruct((copies, *parts.shape[1:]), jnp.float32),
        in_specs=in_vmem(1),
        out_specs=pl.BlockSpec(memory_space=pltpu.VMEM),
        compiler_params=pltpu.CompilerParams(vmem_limit_bytes=4 * 1024 * 1024),
        cost_estimate=pl.CostEstimate(
            flops=parts.size, bytes_accessed=4 * parts.size, transcendentals=0
        ),
    )(parts)


def residual_kernel(ring, pairs_ref, swap_ref, every_ref, out_ref):
    slots, occ, width = out_ref.shape
    group = LANES // ring
    chunks = every_ref.shape[2] // LANES // 2
    lane_group = lax.broadcasted_iota(jnp.int32, (1, LANES), 1) // group

    def half_tile(a_tile, b_tile, c):
        holder = (a_tile // ring * ring + lax.rem(b_tile, ring)) * 2 + c
        first = b_tile // ring * (chunks * LANES)
        found = jnp.zeros((occ, LANES), jnp.float32)
        for m in range(chunks):
            block = every_ref[holder, :, pl.ds(pl.multiple_of(first + m * LANES, LANES), LANES)]
            shift = lax.rem((m + ring - lax.rem(a_tile, ring)) * group, LANES)
            found = jnp.where(lane_group == m, pltpu.roll(block, shift, 1), found)
        return found

    def tiles(role):
        return jnp.concatenate(
            [
                jnp.concatenate(
                    [half_tile(pairs_ref[s, role], pairs_ref[s, 1 - role], c) for c in range(2)],
                    axis=1,
                )
                for s in range(slots)
            ],
            axis=0,
        )

    def placed(rows, spot):
        column = lax.broadcasted_iota(jnp.int32, (width, width), 1)
        chosen = (column == spot).astype(jnp.float32)
        return jnp.dot(
            rows, chosen, preferred_element_type=jnp.float32, precision=lax.Precision.HIGHEST
        )

    lane = lax.broadcasted_iota(jnp.int32, (width, width), 0)
    core_b = lane // LANES
    core_a = lax.rem(lane // (group // 2) + core_b, 2)
    a = core_a * (TS // 2) + lax.rem(lane, TS // 2)
    b = core_b * (TS // 2) + lax.rem(lane, LANES) // group * 2 + lax.rem(lane // (TS // 2), 2)
    straight = placed(tiles(0), a * TS + b)
    mirror = placed(tiles(1), b * TS + a)
    row = lax.broadcasted_iota(jnp.int32, (slots * occ, slots * occ), 0)
    column = lax.broadcasted_iota(jnp.int32, (slots * occ, slots * occ), 1)
    source = row // occ * occ
    for i in range(occ):
        source = source + jnp.where(lax.rem(row, occ) == i, swap_ref[i], 0)
    turned = jnp.dot(
        (column == source).astype(jnp.float32),
        mirror,
        preferred_element_type=jnp.float32,
        precision=lax.Precision.HIGHEST,
    )
    total = straight + turned
    for s in range(slots):
        out_ref[s] = total[s * occ : (s + 1) * occ]


def residual_tiles(pairs, swap, every, ring):
    slots, occ = pairs.shape[0], swap.shape[0]
    return pl.pallas_call(
        functools.partial(residual_kernel, ring),
        out_shape=jax.ShapeDtypeStruct((slots, occ, TS * TS), jnp.float32),
        in_specs=[pl.BlockSpec(memory_space=pltpu.SMEM)] * 2 + in_vmem(1),
        out_specs=pl.BlockSpec(memory_space=pltpu.VMEM),
        compiler_params=pltpu.CompilerParams(vmem_limit_bytes=8 * 1024 * 1024),
        cost_estimate=pl.CostEstimate(
            flops=100 * every.size, bytes_accessed=4 * every.size, transcendentals=0
        ),
    )(pairs, swap, every)


def on_device(chol, amplitudes, tile_pairs, partner, pair_swap):
    out_count = lax.axis_size(OUT)
    con_count = lax.axis_size(CONTRACT)
    ring = lax.axis_size("x")
    a_dev, c_dev, p_size = chol.shape
    i_dev = amplitudes.shape[0]
    i_count = i_dev * out_count
    half = c_dev // 2
    pair_rows = 2 * a_dev

    other_amps = lax.ppermute(amplitudes, "yh", PAIR)
    rows = jnp.transpose(chol.reshape(a_dev, 2, half, p_size), (2, 1, 0, 3))
    extra = jnp.stack([amplitudes, other_amps], axis=0).reshape(2, i_dev, 2, -1)
    extra = jnp.transpose(extra, (0, 2, 1, 3)).reshape(2, pair_rows, -1)
    extra = jnp.pad(extra, ((0, 0), (0, 0), (0, p_size - extra.shape[2])))
    packed = jnp.concatenate([rows.reshape(half, pair_rows, p_size), extra], axis=0)
    near = sent_to_all(packed.reshape(-1, p_size), "x")

    z, yl, yh = lax.axis_index("z"), lax.axis_index("yl"), lax.axis_index("yh")
    depth_z = lax.axis_size("z")
    window = chol.reshape(2, -1, p_size)
    piece = jnp.where(yl == 0, window[0], lax.ppermute(window[1], CONTRACT, [(0, 1)]))
    got = sum(lax.ppermute(piece, "z", [(0, to)]) for to in RELAYS)
    piece = jnp.where(z == 0, piece, got)
    reach = {}
    for to in range(depth_z):
        if to and to not in RELAYS:
            steps = [((to - at + depth_z // 2) % depth_z - depth_z // 2, at) for at in (0, *RELAYS)]
            step, at = min(steps, key=lambda pair: abs(pair[0]))
            reach.setdefault(step, []).append((at, to))
    got = sum(lax.ppermute(piece, "z", reach[step]) for step in sorted(reach, key=abs, reverse=True))
    sender = functools.reduce(jnp.logical_or, [z == at for at in (0, *RELAYS)])
    piece = jnp.where(sender, piece, got)
    quarters = [piece] + [
        lax.ppermute(piece, ("yl", "yh"), [(at, at ^ q) for at in range(4)]) for q in (2, 1, 3)
    ]

    far = lax.ppermute(near, "core", PAIR)
    place = jnp.stack([lax.axis_index("core"), yh, 2 * yh + yl])
    partial = ladder_partials(place, near, far, quarters, 2 * a_dev, i_count, con_count)
    every = exchange(totals(exchange(partial, CONTRACT), out_count), OUT)

    slot_count, occ_dev = tile_pairs.shape[0] // out_count, i_count // con_count
    first = lax.axis_index(OUT) * slot_count
    pairs = lax.dynamic_slice_in_dim(tile_pairs, first, slot_count, 0)
    first = lax.axis_index(CONTRACT) * occ_dev
    swap = lax.dynamic_slice_in_dim(pair_swap, first, occ_dev, 0) - first
    return residual_tiles(pairs, swap, every, ring)


def solution(mesh):
    torus = Mesh(mesh.devices.reshape(16, 2, 2, 4, 2), ("z", "yl", "yh", "x", "core"))
    in_specs = (P(OUT, CONTRACT, None), P(OUT, CONTRACT), P(), P(), P())
    out_specs = P(OUT, CONTRACT, None)

    return jax.shard_map(
        on_device, mesh=torus, in_specs=in_specs, out_specs=out_specs, check_vma=False
    )
```

```python
import functools

import jax
import jax.numpy as jnp
from jax import lax
from jax.experimental import pallas as pl
from jax.experimental.pallas import tpu as pltpu
from jax.sharding import Mesh
from jax.sharding import PartitionSpec as P

TS = 16
LANES = 128
CONTRACT = ("z", "yl")
OUT = ("yh", "x", "core")
PAIR = [(0, 1), (1, 0)]
LONG, MIDDLE = [(0, 3), (0, 13)], [(3, 6), (13, 10)]
SENDERS = (0, 3, 6, 10, 13)


def exchange(array, axes):
    return lax.all_to_all(array, axes, 0, 0, tiled=True)


def sent_to_all(array, axes):
    count = lax.axis_size(axes)
    return exchange(jnp.broadcast_to(array[None], (count, *array.shape)), axes)


def ladder_kernel(place_ref, near_ref, far_ref, *refs):
    *quarter_refs, out_ref, stack_ref, right_ref = refs
    core, yh, own = place_ref[0], place_ref[1], place_ref[2]
    size = quarter_refs[0].shape[0]
    for q, ref in enumerate(quarter_refs):
        right_ref[pl.ds(pl.multiple_of((own ^ q) * size, size), size), :] = ref[...]
    b_count, depth, _ = stack_ref.shape
    ring, pair_rows = near_ref.shape[0], b_count
    c_pairs = near_ref.shape[1] // pair_rows - 2
    a_dev = pair_rows // 2
    d_count = right_ref.shape[0] // b_count
    right = right_ref[...]
    for n in range(0, c_pairs, 2):
        left = jnp.concatenate(
            [
                ref[x, m * pair_rows : (m + 1) * pair_rows, :]
                for m in (n, n + 1)
                for x in range(ring)
                for ref in (near_ref, far_ref)
            ],
            axis=0,
        )
        part = lax.dot_general(
            right, left, (((1,), (1,)), ((), ())), preferred_element_type=jnp.float32
        ).astype(jnp.bfloat16)
        part = part.reshape(b_count, d_count, 2 * LANES)
        for h in range(2):
            rows = (n + h) * d_count
            stack_ref[:, rows : rows + d_count, :] = part[:, :, h * LANES : (h + 1) * LANES]
    amps = jnp.concatenate(
        [
            ref[x, m * pair_rows : (m + 1) * pair_rows, :depth]
            for m in (c_pairs, c_pairs + 1)
            for ref in (near_ref, far_ref)
            for x in range(ring)
        ],
        axis=0,
    )
    blocks = 4 * ring
    odd = lax.rem(lax.broadcasted_iota(jnp.int32, (1, 1, LANES), 2) // a_dev, 2) == 1
    for q in range(b_count // 2):
        sums = []
        for b, step in ((2 * q, LANES - a_dev), (2 * q + 1, a_dev)):
            full = jnp.dot(amps, stack_ref[b], preferred_element_type=jnp.float32)
            full = full.reshape(blocks, 2, a_dev, LANES)
            mixed = jnp.where(odd, full[:, 1], full[:, 0]).reshape(blocks * a_dev, LANES)
            sums.append(mixed + pltpu.roll(mixed, step, 1))
        found = jnp.where(odd[0], sums[1], sums[0]).astype(out_ref.dtype)
        for block in range(blocks):
            other_yh, other_core, x = block // (2 * ring), block // ring % 2, block % ring
            place = (lax.rem(yh + other_yh, 2) * ring + x) * 2 + lax.rem(core + other_core, 2)
            for h in range(2):
                rows = found[block * a_dev + h * (a_dev // 2) : block * a_dev + (h + 1) * (a_dev // 2)]
                out_ref[2 * place + h, :, q * LANES : (q + 1) * LANES] = rows


def in_vmem(count):
    return [pl.BlockSpec(memory_space=pltpu.VMEM)] * count


def ladder_partials(place, near, far, quarters, b_count, i_count, con_count):
    right = (len(quarters) * quarters[0].shape[0], quarters[0].shape[1])
    depth = (near.shape[1] // b_count - 2) * (right[0] // b_count)
    pairs = 2 * near.size * right[0]
    return pl.pallas_call(
        ladder_kernel,
        out_shape=jax.ShapeDtypeStruct(
            (con_count, i_count // con_count, b_count * LANES // 2), jnp.bfloat16
        ),
        in_specs=[pl.BlockSpec(memory_space=pltpu.SMEM)] + in_vmem(2 + len(quarters)),
        out_specs=pl.BlockSpec(memory_space=pltpu.VMEM),
        scratch_shapes=[
            pltpu.VMEM((b_count, depth, LANES), jnp.bfloat16),
            pltpu.VMEM(right, jnp.bfloat16),
        ],
        compiler_params=pltpu.CompilerParams(vmem_limit_bytes=12 * 1024 * 1024),
        cost_estimate=pl.CostEstimate(
            flops=2 * pairs, bytes_accessed=4 * near.size, transcendentals=0
        ),
    )(place, near, far, *quarters)


def total_kernel(parts_ref, out_ref):
    total = parts_ref[0].astype(jnp.float32)
    for k in range(1, parts_ref.shape[0]):
        total = total + parts_ref[k].astype(jnp.float32)
    for o in range(out_ref.shape[0]):
        out_ref[o] = total


def totals(parts, copies):
    return pl.pallas_call(
        total_kernel,
        out_shape=jax.ShapeDtypeStruct((copies, *parts.shape[1:]), jnp.float32),
        in_specs=in_vmem(1),
        out_specs=pl.BlockSpec(memory_space=pltpu.VMEM),
        compiler_params=pltpu.CompilerParams(vmem_limit_bytes=4 * 1024 * 1024),
        cost_estimate=pl.CostEstimate(
            flops=parts.size, bytes_accessed=4 * parts.size, transcendentals=0
        ),
    )(parts)


def residual_kernel(ring, pairs_ref, swap_ref, every_ref, out_ref):
    slots, occ, width = out_ref.shape
    group = LANES // ring
    chunks = every_ref.shape[2] // LANES // 2
    lane_group = lax.broadcasted_iota(jnp.int32, (1, LANES), 1) // group

    def half_tile(a_tile, b_tile, c):
        holder = (a_tile // ring * ring + lax.rem(b_tile, ring)) * 2 + c
        first = b_tile // ring * (chunks * LANES)
        found = jnp.zeros((occ, LANES), jnp.float32)
        for m in range(chunks):
            block = every_ref[holder, :, pl.ds(pl.multiple_of(first + m * LANES, LANES), LANES)]
            shift = lax.rem((m + ring - lax.rem(a_tile, ring)) * group, LANES)
            found = jnp.where(lane_group == m, pltpu.roll(block, shift, 1), found)
        return found

    def tiles(role):
        return jnp.concatenate(
            [
                jnp.concatenate(
                    [half_tile(pairs_ref[s, role], pairs_ref[s, 1 - role], c) for c in range(2)],
                    axis=1,
                )
                for s in range(slots)
            ],
            axis=0,
        )

    def thirds(rows):
        high = rows.astype(jnp.bfloat16)
        rest = rows - high.astype(jnp.float32)
        middle = rest.astype(jnp.bfloat16)
        low = (rest - middle.astype(jnp.float32)).astype(jnp.bfloat16)
        return high, middle, low

    def placed(parts, spot):
        column = lax.broadcasted_iota(jnp.int32, (width, width), 1)
        chosen = (column == spot).astype(jnp.float32).astype(jnp.bfloat16)
        found = jnp.dot(
            jnp.concatenate(parts, axis=0), chosen, preferred_element_type=jnp.float32
        )
        high, middle, low = (found[n * slots * occ : (n + 1) * slots * occ] for n in range(3))
        return high + middle + low

    lane = lax.broadcasted_iota(jnp.int32, (width, width), 0)
    core_b = lane // LANES
    core_a = lax.rem(lane // (group // 2) + core_b, 2)
    a = core_a * (TS // 2) + lax.rem(lane, TS // 2)
    b = core_b * (TS // 2) + lax.rem(lane, LANES) // group * 2 + lax.rem(lane // (TS // 2), 2)
    straight = placed(thirds(tiles(0)), a * TS + b)
    row = lax.broadcasted_iota(jnp.int32, (slots * occ, slots * occ), 0)
    column = lax.broadcasted_iota(jnp.int32, (slots * occ, slots * occ), 1)
    source = row // occ * occ
    for i in range(occ):
        source = source + jnp.where(lax.rem(row, occ) == i, swap_ref[i], 0)
    chosen = (column == source).astype(jnp.float32).astype(jnp.bfloat16)
    swapped = [
        jnp.dot(chosen, part, preferred_element_type=jnp.float32).astype(jnp.bfloat16)
        for part in thirds(tiles(1))
    ]
    total = straight + placed(swapped, b * TS + a)
    for s in range(slots):
        out_ref[s] = total[s * occ : (s + 1) * occ]


def residual_tiles(pairs, swap, every, ring):
    slots, occ = pairs.shape[0], swap.shape[0]
    return pl.pallas_call(
        functools.partial(residual_kernel, ring),
        out_shape=jax.ShapeDtypeStruct((slots, occ, TS * TS), jnp.float32),
        in_specs=[pl.BlockSpec(memory_space=pltpu.SMEM)] * 2 + in_vmem(1),
        out_specs=pl.BlockSpec(memory_space=pltpu.VMEM),
        compiler_params=pltpu.CompilerParams(vmem_limit_bytes=8 * 1024 * 1024),
        cost_estimate=pl.CostEstimate(
            flops=100 * every.size, bytes_accessed=4 * every.size, transcendentals=0
        ),
    )(pairs, swap, every)


def on_device(chol, amplitudes, tile_pairs, partner, pair_swap):
    out_count = lax.axis_size(OUT)
    con_count = lax.axis_size(CONTRACT)
    ring = lax.axis_size("x")
    a_dev, c_dev, p_size = chol.shape
    i_dev = amplitudes.shape[0]
    i_count = i_dev * out_count
    half = c_dev // 2
    pair_rows = 2 * a_dev

    other_amps = lax.ppermute(amplitudes, "yh", PAIR)
    rows = jnp.transpose(chol.reshape(a_dev, 2, half, p_size), (2, 1, 0, 3))
    extra = jnp.stack([amplitudes, other_amps], axis=0).reshape(2, i_dev, 2, -1)
    extra = jnp.transpose(extra, (0, 2, 1, 3)).reshape(2, pair_rows, -1)
    extra = jnp.pad(extra, ((0, 0), (0, 0), (0, p_size - extra.shape[2])))
    packed = jnp.concatenate([rows.reshape(half, pair_rows, p_size), extra], axis=0)
    near = sent_to_all(packed.reshape(-1, p_size), "x")

    z, yl, yh = lax.axis_index("z"), lax.axis_index("yl"), lax.axis_index("yh")
    depth_z = lax.axis_size("z")
    window = chol.reshape(2, -1, p_size)
    piece = jnp.where(yl == 0, window[0], lax.ppermute(window[1], CONTRACT, [(0, 1)]))
    got = sum(lax.ppermute(piece, "z", [hop]) for hop in LONG)
    piece = jnp.where(z == 0, piece, got)
    got = lax.ppermute(piece, "z", MIDDLE)
    piece = jnp.where(functools.reduce(jnp.logical_or, [z == to for _, to in MIDDLE]), got, piece)
    reach = {}
    for to in range(depth_z):
        if to not in SENDERS:
            steps = [((to - at + depth_z // 2) % depth_z - depth_z // 2, at) for at in SENDERS]
            step, at = min(steps, key=lambda pair: abs(pair[0]))
            reach.setdefault(step, []).append((at, to))
    steps = sorted(reach, key=abs, reverse=True)
    got = lax.ppermute(piece, "z", reach[steps[0]])
    got = sum((lax.ppermute(piece, "z", reach[step]) for step in steps[1:]), got)
    sender = functools.reduce(jnp.logical_or, [z == at for at in SENDERS])
    piece = jnp.where(sender, piece, got)
    quarters = [piece] + [
        lax.ppermute(piece, ("yl", "yh"), [(at, at ^ q) for at in range(4)]) for q in (2, 1, 3)
    ]

    far = lax.ppermute(near, "core", PAIR)
    place = jnp.stack([lax.axis_index("core"), yh, 2 * yh + yl])
    partial = ladder_partials(place, near, far, quarters, 2 * a_dev, i_count, con_count)
    every = exchange(totals(exchange(partial, CONTRACT), out_count), OUT)

    slot_count, occ_dev = tile_pairs.shape[0] // out_count, i_count // con_count
    first = lax.axis_index(OUT) * slot_count
    pairs = lax.dynamic_slice_in_dim(tile_pairs, first, slot_count, 0)
    first = lax.axis_index(CONTRACT) * occ_dev
    swap = lax.dynamic_slice_in_dim(pair_swap, first, occ_dev, 0) - first
    return residual_tiles(pairs, swap, every, ring)


def solution(mesh):
    torus = Mesh(mesh.devices.reshape(16, 2, 2, 4, 2), ("z", "yl", "yh", "x", "core"))
    in_specs = (P(OUT, CONTRACT, None), P(OUT, CONTRACT), P(), P(), P())
    out_specs = P(OUT, CONTRACT, None)

    return jax.shard_map(
        on_device, mesh=torus, in_specs=in_specs, out_specs=out_specs, check_vma=False
    )
```

```python
import functools

import jax
import jax.numpy as jnp
from jax import lax
from jax.experimental import pallas as pl
from jax.experimental.pallas import tpu as pltpu
from jax.sharding import Mesh
from jax.sharding import PartitionSpec as P

TS = 16
LANES = 128
CONTRACT = ("z", "yl")
OUT = ("yh", "x", "core")
PAIR = [(0, 1), (1, 0)]
LONG, MIDDLE = [(0, 3), (0, 13)], [(3, 6), (13, 10)]
SENDERS = (0, 3, 6, 10, 13)


def exchange(array, axes):
    return lax.all_to_all(array, axes, 0, 0, tiled=True)


def sent_to_all(array, axes):
    count = lax.axis_size(axes)
    return exchange(jnp.broadcast_to(array[None], (count, *array.shape)), axes)


def ladder_kernel(place_ref, near_ref, far_ref, amps_ref, right_ref, out_ref, stack_ref):
    b_count, depth, _ = stack_ref.shape
    ring, pair_rows = near_ref.shape[0], b_count
    c_pairs = near_ref.shape[1] // pair_rows
    a_dev = pair_rows // 2
    order = [lax.rem(place_ref[0] + ring - x, ring) for x in range(ring)]
    d_count = right_ref.shape[0] // b_count
    right = right_ref[...]
    for n in range(0, c_pairs, 2):
        left = jnp.concatenate(
            [
                ref[order[x], m * pair_rows : (m + 1) * pair_rows, :]
                for m in (n, n + 1)
                for x in range(ring)
                for ref in (near_ref, far_ref)
            ],
            axis=0,
        )
        part = lax.dot_general(
            right, left, (((1,), (1,)), ((), ())), preferred_element_type=jnp.float32
        ).astype(jnp.bfloat16)
        part = part.reshape(b_count, d_count, 2 * LANES)
        for h in range(2):
            rows = (n + h) * d_count
            stack_ref[:, rows : rows + d_count, :] = part[:, :, h * LANES : (h + 1) * LANES]
    i_count = amps_ref.shape[0]
    amps = jnp.concatenate([amps_ref[:, :depth], amps_ref[:, depth:]], axis=0)
    odd = lax.rem(lax.broadcasted_iota(jnp.int32, (1, LANES), 1) // a_dev, 2) == 1
    rows = out_ref.shape[1]
    for q in range(b_count // 2):
        sums = []
        for b, step in ((2 * q, LANES - a_dev), (2 * q + 1, a_dev)):
            full = jnp.dot(amps, stack_ref[b], preferred_element_type=jnp.float32)
            mixed = jnp.where(odd, full[i_count:], full[:i_count])
            sums.append(mixed + pltpu.roll(mixed, step, 1))
        found = jnp.where(odd, sums[1], sums[0]).astype(out_ref.dtype)
        for k in range(out_ref.shape[0]):
            out_ref[k, :, q * LANES : (q + 1) * LANES] = found[k * rows : (k + 1) * rows]


def in_vmem(count):
    return [pl.BlockSpec(memory_space=pltpu.VMEM)] * count


def ladder_partials(place, near, far, amps, right, b_count, con_count):
    i_count = amps.shape[0]
    pairs = 2 * near.size * right.shape[0]
    return pl.pallas_call(
        ladder_kernel,
        out_shape=jax.ShapeDtypeStruct(
            (con_count, i_count // con_count, b_count * LANES // 2), jnp.bfloat16
        ),
        in_specs=[pl.BlockSpec(memory_space=pltpu.SMEM)] + in_vmem(4),
        out_specs=pl.BlockSpec(memory_space=pltpu.VMEM),
        scratch_shapes=[pltpu.VMEM((b_count, amps.shape[1] // 2, LANES), jnp.bfloat16)],
        compiler_params=pltpu.CompilerParams(vmem_limit_bytes=12 * 1024 * 1024),
        cost_estimate=pl.CostEstimate(
            flops=2 * pairs, bytes_accessed=4 * near.size, transcendentals=0
        ),
    )(place, near, far, amps, right)


def total_kernel(parts_ref, out_ref):
    total = parts_ref[0].astype(jnp.float32)
    for k in range(1, parts_ref.shape[0]):
        total = total + parts_ref[k].astype(jnp.float32)
    for o in range(out_ref.shape[0]):
        out_ref[o] = total


def totals(parts, copies):
    return pl.pallas_call(
        total_kernel,
        out_shape=jax.ShapeDtypeStruct((copies, *parts.shape[1:]), jnp.float32),
        in_specs=in_vmem(1),
        out_specs=pl.BlockSpec(memory_space=pltpu.VMEM),
        compiler_params=pltpu.CompilerParams(vmem_limit_bytes=4 * 1024 * 1024),
        cost_estimate=pl.CostEstimate(
            flops=parts.size, bytes_accessed=4 * parts.size, transcendentals=0
        ),
    )(parts)


def residual_kernel(ring, pairs_ref, swap_ref, every_ref, out_ref):
    slots, occ, width = out_ref.shape
    group = LANES // ring
    chunks = every_ref.shape[2] // LANES // 2
    lane_group = lax.broadcasted_iota(jnp.int32, (1, LANES), 1) // group

    def half_tile(a_tile, b_tile, c):
        holder = (a_tile // ring * ring + lax.rem(b_tile, ring)) * 2 + c
        first = b_tile // ring * (chunks * LANES)
        found = jnp.zeros((occ, LANES), jnp.float32)
        for m in range(chunks):
            block = every_ref[holder, :, pl.ds(pl.multiple_of(first + m * LANES, LANES), LANES)]
            shift = lax.rem((m + ring - lax.rem(a_tile, ring)) * group, LANES)
            found = jnp.where(lane_group == m, pltpu.roll(block, shift, 1), found)
        return found

    def tiles(role):
        return jnp.concatenate(
            [
                jnp.concatenate(
                    [half_tile(pairs_ref[s, role], pairs_ref[s, 1 - role], c) for c in range(2)],
                    axis=1,
                )
                for s in range(slots)
            ],
            axis=0,
        )

    def thirds(rows):
        high = rows.astype(jnp.bfloat16)
        rest = rows - high.astype(jnp.float32)
        middle = rest.astype(jnp.bfloat16)
        low = (rest - middle.astype(jnp.float32)).astype(jnp.bfloat16)
        return high, middle, low

    def placed(parts, spot):
        column = lax.broadcasted_iota(jnp.int32, (width, width), 1)
        chosen = (column == spot).astype(jnp.float32).astype(jnp.bfloat16)
        found = jnp.dot(
            jnp.concatenate(parts, axis=0), chosen, preferred_element_type=jnp.float32
        )
        high, middle, low = (found[n * slots * occ : (n + 1) * slots * occ] for n in range(3))
        return high + middle + low

    lane = lax.broadcasted_iota(jnp.int32, (width, width), 0)
    core_b = lane // LANES
    core_a = lax.rem(lane // (group // 2) + core_b, 2)
    a = core_a * (TS // 2) + lax.rem(lane, TS // 2)
    b = core_b * (TS // 2) + lax.rem(lane, LANES) // group * 2 + lax.rem(lane // (TS // 2), 2)
    straight = placed(thirds(tiles(0)), a * TS + b)
    row = lax.broadcasted_iota(jnp.int32, (slots * occ, slots * occ), 0)
    column = lax.broadcasted_iota(jnp.int32, (slots * occ, slots * occ), 1)
    source = row // occ * occ
    for i in range(occ):
        source = source + jnp.where(lax.rem(row, occ) == i, swap_ref[i], 0)
    chosen = (column == source).astype(jnp.float32).astype(jnp.bfloat16)
    swapped = [
        jnp.dot(chosen, part, preferred_element_type=jnp.float32).astype(jnp.bfloat16)
        for part in thirds(tiles(1))
    ]
    total = straight + placed(swapped, b * TS + a)
    for s in range(slots):
        out_ref[s] = total[s * occ : (s + 1) * occ]


def residual_tiles(pairs, swap, every, ring):
    slots, occ = pairs.shape[0], swap.shape[0]
    return pl.pallas_call(
        functools.partial(residual_kernel, ring),
        out_shape=jax.ShapeDtypeStruct((slots, occ, TS * TS), jnp.float32),
        in_specs=[pl.BlockSpec(memory_space=pltpu.SMEM)] * 2 + in_vmem(1),
        out_specs=pl.BlockSpec(memory_space=pltpu.VMEM),
        compiler_params=pltpu.CompilerParams(vmem_limit_bytes=8 * 1024 * 1024),
        cost_estimate=pl.CostEstimate(
            flops=100 * every.size, bytes_accessed=4 * every.size, transcendentals=0
        ),
    )(pairs, swap, every)


def on_device(chol, amplitudes, tile_pairs, partner, pair_swap):
    out_count = lax.axis_size(OUT)
    con_count = lax.axis_size(CONTRACT)
    ring = lax.axis_size("x")
    a_dev, c_dev, p_size = chol.shape
    i_count = amplitudes.shape[0] * out_count
    half = c_dev // 2

    rows = jnp.transpose(chol.reshape(a_dev, 2, half, p_size), (2, 1, 0, 3))
    rows = rows.reshape(-1, p_size)
    near = [rows] + [
        lax.ppermute(rows, "x", [(x, (x + shift) % ring) for x in range(ring)])
        for shift in range(1, ring)
    ]
    amps = sent_to_all(amplitudes, OUT).reshape(i_count, -1)

    z, yl = lax.axis_index("z"), lax.axis_index("yl")
    depth_z = lax.axis_size("z")
    window = chol.reshape(2, -1, p_size)
    piece = jnp.where(yl == 0, window[0], lax.ppermute(window[1], CONTRACT, [(0, 1)]))
    got = sum(lax.ppermute(piece, "z", [hop]) for hop in LONG)
    piece = jnp.where(z == 0, piece, got)
    got = lax.ppermute(piece, "z", MIDDLE)
    piece = jnp.where(functools.reduce(jnp.logical_or, [z == to for _, to in MIDDLE]), got, piece)
    reach = {}
    for to in range(depth_z):
        if to not in SENDERS:
            steps = [((to - at + depth_z // 2) % depth_z - depth_z // 2, at) for at in SENDERS]
            step, at = min(steps, key=lambda pair: abs(pair[0]))
            reach.setdefault(step, []).append((at, to))
    steps = sorted(reach, key=abs, reverse=True)
    got = lax.ppermute(piece, "z", reach[steps[0]])
    got = sum((lax.ppermute(piece, "z", reach[step]) for step in steps[1:]), got)
    sender = functools.reduce(jnp.logical_or, [z == at for at in SENDERS])
    piece = jnp.where(sender, piece, got)
    right = sent_to_all(piece, ("yh", "yl")).reshape(-1, p_size)

    near = jnp.stack(near, axis=0)
    far = lax.ppermute(near, "core", PAIR)

    place = lax.axis_index("x").reshape(1)
    partial = ladder_partials(place, near, far, amps, right, 2 * a_dev, con_count)
    every = exchange(totals(exchange(partial, CONTRACT), out_count), OUT)

    slot_count, occ_dev = tile_pairs.shape[0] // out_count, i_count // con_count
    first = lax.axis_index(OUT) * slot_count
    pairs = lax.dynamic_slice_in_dim(tile_pairs, first, slot_count, 0)
    first = lax.axis_index(CONTRACT) * occ_dev
    swap = lax.dynamic_slice_in_dim(pair_swap, first, occ_dev, 0) - first
    return residual_tiles(pairs, swap, every, ring)


def solution(mesh):
    torus = Mesh(mesh.devices.reshape(16, 2, 2, 4, 2), ("z", "yl", "yh", "x", "core"))
    in_specs = (P(OUT, CONTRACT, None), P(OUT, CONTRACT), P(), P(), P())
    out_specs = P(OUT, CONTRACT, None)

    return jax.shard_map(
        on_device, mesh=torus, in_specs=in_specs, out_specs=out_specs, check_vma=False
    )
```

```python
import functools

import jax
import jax.numpy as jnp
from jax import lax
from jax.experimental import pallas as pl
from jax.experimental.pallas import tpu as pltpu
from jax.sharding import Mesh
from jax.sharding import PartitionSpec as P

TS = 16
LANES = 128
CONTRACT = ("z", "yl")
OUT = ("yh", "x", "core")
PAIR = [(0, 1), (1, 0)]
LONG, MIDDLE = [(0, 3), (0, 13)], [(3, 6), (13, 10)]
SENDERS = (0, 3, 6, 10, 13)


def exchange(array, axes):
    return lax.all_to_all(array, axes, 0, 0, tiled=True)


def ladder_kernel(place_ref, near_ref, far_ref, *refs):
    *quarter_refs, out_ref, stack_ref, right_ref, amps_ref = refs
    core, yh, own = place_ref[0], place_ref[1], place_ref[2]
    size = quarter_refs[0].shape[0]
    for q, ref in enumerate(quarter_refs):
        right_ref[pl.ds(pl.multiple_of((own ^ q) * size, size), size), :] = ref[...]
    b_count, depth, _ = stack_ref.shape
    ring, pair_rows = near_ref.shape[0], b_count
    c_pairs = near_ref.shape[1] // pair_rows - 2
    a_dev = pair_rows // 2
    d_count = right_ref.shape[0] // b_count
    right = right_ref[...]
    for n in range(0, c_pairs, 2):
        left = jnp.concatenate(
            [
                ref[x, m * pair_rows : (m + 1) * pair_rows, :]
                for m in (n, n + 1)
                for x in range(ring)
                for ref in (near_ref, far_ref)
            ],
            axis=0,
        )
        part = lax.dot_general(
            right, left, (((1,), (1,)), ((), ())), preferred_element_type=jnp.float32
        ).astype(jnp.bfloat16)
        part = part.reshape(b_count, d_count, 2 * LANES)
        for h in range(2):
            rows = (n + h) * d_count
            stack_ref[:, rows : rows + d_count, :] = part[:, :, h * LANES : (h + 1) * LANES]
    for m in range(2):
        for rc, ref in enumerate((near_ref, far_ref)):
            for x in range(ring):
                place = (lax.rem(yh + m, 2) * ring + x) * 2 + lax.rem(core + rc, 2)
                first = (c_pairs + m) * pair_rows
                block = ref[x, first : first + pair_rows, :depth].astype(jnp.float32)
                for g in range(2):
                    amps_ref[g, place] = block[g * a_dev : (g + 1) * a_dev]
    i_count = amps_ref.shape[1] * a_dev
    amps = amps_ref[...].reshape(2 * i_count, depth).astype(jnp.bfloat16)
    odd = lax.rem(lax.broadcasted_iota(jnp.int32, (1, LANES), 1) // a_dev, 2) == 1
    rows = out_ref.shape[1]
    for q in range(b_count // 2):
        sums = []
        for b, step in ((2 * q, LANES - a_dev), (2 * q + 1, a_dev)):
            full = jnp.dot(amps, stack_ref[b], preferred_element_type=jnp.float32)
            mixed = jnp.where(odd, full[i_count:], full[:i_count])
            sums.append(mixed + pltpu.roll(mixed, step, 1))
        found = jnp.where(odd, sums[1], sums[0]).astype(out_ref.dtype)
        for k in range(out_ref.shape[0]):
            out_ref[k, :, q * LANES : (q + 1) * LANES] = found[k * rows : (k + 1) * rows]


def in_vmem(count):
    return [pl.BlockSpec(memory_space=pltpu.VMEM)] * count


def ladder_partials(place, near, far, quarters, b_count, i_count, con_count):
    right = (len(quarters) * quarters[0].shape[0], quarters[0].shape[1])
    depth = (near.shape[1] // b_count - 2) * (right[0] // b_count)
    pairs = 2 * near.size * right[0]
    return pl.pallas_call(
        ladder_kernel,
        out_shape=jax.ShapeDtypeStruct(
            (con_count, i_count // con_count, b_count * LANES // 2), jnp.bfloat16
        ),
        in_specs=[pl.BlockSpec(memory_space=pltpu.SMEM)] + in_vmem(2 + len(quarters)),
        out_specs=pl.BlockSpec(memory_space=pltpu.VMEM),
        scratch_shapes=[
            pltpu.VMEM((b_count, depth, LANES), jnp.bfloat16),
            pltpu.VMEM(right, jnp.bfloat16),
            pltpu.VMEM((2, 4 * near.shape[0], b_count // 2, depth), jnp.float32),
        ],
        compiler_params=pltpu.CompilerParams(vmem_limit_bytes=12 * 1024 * 1024),
        cost_estimate=pl.CostEstimate(
            flops=2 * pairs, bytes_accessed=4 * near.size, transcendentals=0
        ),
    )(place, near, far, *quarters)


def pack_kernel(rows_ref, amps_ref, other_ref, out_ref):
    count, cells = rows_ref.shape[0], amps_ref.shape[1] // 2
    for n in range(out_ref.shape[0]):
        out_ref[n, :count, :] = rows_ref[...]
    out_ref[:, count:, cells:] = jnp.zeros_like(out_ref[:, count:, cells:])
    for m, ref in enumerate((amps_ref, other_ref)):
        block = jnp.concatenate([ref[:, :cells], ref[:, cells:]], axis=0)
        for n in range(out_ref.shape[0]):
            first = count + m * block.shape[0]
            out_ref[n, first : first + block.shape[0], :cells] = block


def packed_copies(rows, amps, other, copies):
    count = rows.shape[0] + 4 * amps.shape[0]
    return pl.pallas_call(
        pack_kernel,
        out_shape=jax.ShapeDtypeStruct((copies, count, rows.shape[1]), rows.dtype),
        in_specs=in_vmem(3),
        out_specs=pl.BlockSpec(memory_space=pltpu.VMEM),
        compiler_params=pltpu.CompilerParams(vmem_limit_bytes=6 * 1024 * 1024),
        cost_estimate=pl.CostEstimate(
            flops=rows.size, bytes_accessed=16 * rows.size, transcendentals=0
        ),
    )(rows, amps, other)


def total_kernel(parts_ref, out_ref):
    total = parts_ref[0].astype(jnp.float32)
    for k in range(1, parts_ref.shape[0]):
        total = total + parts_ref[k].astype(jnp.float32)
    total = total.astype(out_ref.dtype)
    for o in range(out_ref.shape[0]):
        out_ref[o] = total


def totals(parts, copies):
    return pl.pallas_call(
        total_kernel,
        out_shape=jax.ShapeDtypeStruct((copies, *parts.shape[1:]), parts.dtype),
        in_specs=in_vmem(1),
        out_specs=pl.BlockSpec(memory_space=pltpu.VMEM),
        compiler_params=pltpu.CompilerParams(vmem_limit_bytes=4 * 1024 * 1024),
        cost_estimate=pl.CostEstimate(
            flops=parts.size, bytes_accessed=4 * parts.size, transcendentals=0
        ),
    )(parts)


def residual_kernel(ring, pairs_ref, swap_ref, every_ref, out_ref):
    slots, occ, width = out_ref.shape
    group = LANES // ring
    chunks = every_ref.shape[2] // LANES // 2
    lane_group = lax.broadcasted_iota(jnp.int32, (1, LANES), 1) // group

    def half_tile(a_tile, b_tile, c):
        holder = (a_tile // ring * ring + lax.rem(b_tile, ring)) * 2 + c
        first = b_tile // ring * (chunks * LANES)
        found = jnp.zeros((occ, LANES), jnp.float32)
        for m in range(chunks):
            block = every_ref[holder, :, pl.ds(pl.multiple_of(first + m * LANES, LANES), LANES)]
            block = block.astype(jnp.float32)
            shift = lax.rem((m + ring - lax.rem(a_tile, ring)) * group, LANES)
            found = jnp.where(lane_group == m, pltpu.roll(block, shift, 1), found)
        return found

    def tiles(role):
        return jnp.concatenate(
            [
                jnp.concatenate(
                    [half_tile(pairs_ref[s, role], pairs_ref[s, 1 - role], c) for c in range(2)],
                    axis=1,
                )
                for s in range(slots)
            ],
            axis=0,
        ).astype(jnp.bfloat16)

    def placed(rows, spot):
        column = lax.broadcasted_iota(jnp.int32, (width, width), 1)
        chosen = (column == spot).astype(jnp.float32).astype(jnp.bfloat16)
        return jnp.dot(rows, chosen, preferred_element_type=jnp.float32)

    lane = lax.broadcasted_iota(jnp.int32, (width, width), 0)
    core_b = lane // LANES
    core_a = lax.rem(lane // (group // 2) + core_b, 2)
    a = core_a * (TS // 2) + lax.rem(lane, TS // 2)
    b = core_b * (TS // 2) + lax.rem(lane, LANES) // group * 2 + lax.rem(lane // (TS // 2), 2)
    straight = placed(tiles(0), a * TS + b)
    row = lax.broadcasted_iota(jnp.int32, (slots * occ, slots * occ), 0)
    column = lax.broadcasted_iota(jnp.int32, (slots * occ, slots * occ), 1)
    source = row // occ * occ
    for i in range(occ):
        source = source + jnp.where(lax.rem(row, occ) == i, swap_ref[i], 0)
    chosen = (column == source).astype(jnp.float32).astype(jnp.bfloat16)
    swapped = jnp.dot(chosen, tiles(1), preferred_element_type=jnp.float32).astype(jnp.bfloat16)
    total = straight + placed(swapped, b * TS + a)
    for s in range(slots):
        out_ref[s] = total[s * occ : (s + 1) * occ]


def residual_tiles(pairs, swap, every, ring):
    slots, occ = pairs.shape[0], swap.shape[0]
    return pl.pallas_call(
        functools.partial(residual_kernel, ring),
        out_shape=jax.ShapeDtypeStruct((slots, occ, TS * TS), jnp.float32),
        in_specs=[pl.BlockSpec(memory_space=pltpu.SMEM)] * 2 + in_vmem(1),
        out_specs=pl.BlockSpec(memory_space=pltpu.VMEM),
        compiler_params=pltpu.CompilerParams(vmem_limit_bytes=8 * 1024 * 1024),
        cost_estimate=pl.CostEstimate(
            flops=100 * every.size, bytes_accessed=4 * every.size, transcendentals=0
        ),
    )(pairs, swap, every)


def on_device(chol, amplitudes, tile_pairs, partner, pair_swap):
    out_count = lax.axis_size(OUT)
    con_count = lax.axis_size(CONTRACT)
    ring = lax.axis_size("x")
    a_dev, c_dev, p_size = chol.shape
    i_count = amplitudes.shape[0] * out_count
    half = c_dev // 2

    other_amps = lax.ppermute(amplitudes, "yh", PAIR)
    rows = jnp.transpose(chol.reshape(a_dev, 2, half, p_size), (2, 1, 0, 3))
    packed = packed_copies(rows.reshape(-1, p_size), amplitudes, other_amps, ring)
    near = exchange(packed, "x")

    z, yl, yh = lax.axis_index("z"), lax.axis_index("yl"), lax.axis_index("yh")
    depth_z = lax.axis_size("z")
    window = chol.reshape(2, -1, p_size)
    piece = jnp.where(yl == 0, window[0], lax.ppermute(window[1], CONTRACT, [(0, 1)]))
    got = sum(lax.ppermute(piece, "z", [hop]) for hop in LONG)
    piece = jnp.where(z == 0, piece, got)
    got = lax.ppermute(piece, "z", MIDDLE)
    piece = jnp.where(functools.reduce(jnp.logical_or, [z == to for _, to in MIDDLE]), got, piece)
    reach = {}
    for to in range(depth_z):
        if to not in SENDERS:
            steps = [((to - at + depth_z // 2) % depth_z - depth_z // 2, at) for at in SENDERS]
            step, at = min(steps, key=lambda pair: abs(pair[0]))
            reach.setdefault(step, []).append((at, to))
    steps = sorted(reach, key=abs, reverse=True)
    got = lax.ppermute(piece, "z", reach[steps[0]])
    got = sum((lax.ppermute(piece, "z", reach[step]) for step in steps[1:]), got)
    sender = functools.reduce(jnp.logical_or, [z == at for at in SENDERS])
    piece = jnp.where(sender, piece, got)
    quarters = [piece] + [
        lax.ppermute(piece, ("yl", "yh"), [(at, at ^ q) for at in range(4)]) for q in (2, 1, 3)
    ]

    far = lax.ppermute(near, "core", PAIR)
    place = jnp.stack([lax.axis_index("core"), yh, 2 * yh + yl])
    partial = ladder_partials(place, near, far, quarters, 2 * a_dev, i_count, con_count)
    every = exchange(totals(exchange(partial, CONTRACT), out_count), OUT)

    slot_count, occ_dev = tile_pairs.shape[0] // out_count, i_count // con_count
    first = lax.axis_index(OUT) * slot_count
    pairs = lax.dynamic_slice_in_dim(tile_pairs, first, slot_count, 0)
    first = lax.axis_index(CONTRACT) * occ_dev
    swap = lax.dynamic_slice_in_dim(pair_swap, first, occ_dev, 0) - first
    return residual_tiles(pairs, swap, every, ring)


def solution(mesh):
    torus = Mesh(mesh.devices.reshape(16, 2, 2, 4, 2), ("z", "yl", "yh", "x", "core"))
    in_specs = (P(OUT, CONTRACT, None), P(OUT, CONTRACT), P(), P(), P())
    out_specs = P(OUT, CONTRACT, None)

    return jax.shard_map(
        on_device, mesh=torus, in_specs=in_specs, out_specs=out_specs, check_vma=False
    )
```

```python
import functools

import jax
import jax.numpy as jnp
from jax import lax
from jax.experimental import pallas as pl
from jax.experimental.pallas import tpu as pltpu
from jax.sharding import Mesh
from jax.sharding import PartitionSpec as P

TS = 16
LANES = 128
CONTRACT = ("z", "yl")
OUT = ("yh", "x", "core")
PAIR = [(0, 1), (1, 0)]
LONG, MIDDLE = [(0, 3), (0, 12)], [(3, 6), (12, 9), (0, 14)]
SENDERS, HOLDERS = (0, 3, 6, 9, 12), (0, 3, 6, 9, 12, 14)


def exchange(array, axes):
    return lax.all_to_all(array, axes, 0, 0, tiled=True)


def ladder_kernel(place_ref, near_ref, far_ref, *refs):
    *quarter_refs, out_ref, stack_ref, right_ref = refs
    core, yh, own = place_ref[0], place_ref[1], place_ref[2]
    size = quarter_refs[0].shape[0]
    for q, ref in enumerate(quarter_refs):
        right_ref[pl.ds(pl.multiple_of((own ^ q) * size, size), size), :] = ref[...]
    b_count, depth, _ = stack_ref.shape
    ring, pair_rows = near_ref.shape[0], b_count
    c_pairs = near_ref.shape[1] // pair_rows - 2
    a_dev = pair_rows // 2
    d_count = right_ref.shape[0] // b_count
    right = right_ref[...]
    for n in range(0, c_pairs, 2):
        left = jnp.concatenate(
            [
                ref[x, m * pair_rows : (m + 1) * pair_rows, :]
                for m in (n, n + 1)
                for x in range(ring)
                for ref in (near_ref, far_ref)
            ],
            axis=0,
        )
        part = lax.dot_general(
            right, left, (((1,), (1,)), ((), ())), preferred_element_type=jnp.float32
        ).astype(jnp.bfloat16)
        part = part.reshape(b_count, d_count, 2 * LANES)
        for h in range(2):
            rows = (n + h) * d_count
            stack_ref[:, rows : rows + d_count, :] = part[:, :, h * LANES : (h + 1) * LANES]
    held = jnp.concatenate(
        [
            ref[x, m * pair_rows : (m + 1) * pair_rows, :depth]
            for m in (c_pairs, c_pairs + 1)
            for ref in (near_ref, far_ref)
            for x in range(ring)
        ],
        axis=0,
    )
    count = held.shape[0]
    i_count = count // 2
    row = lax.broadcasted_iota(jnp.int32, (count, 1), 0)
    block = lax.rem(row, i_count) // a_dev
    from_yh = lax.rem(block // (2 * ring) + yh, 2)
    from_core = lax.rem(block + core, 2)
    from_x = lax.rem(block // 2, ring)
    source = ((from_yh * 2 + from_core) * ring + from_x) * 2 + row // i_count
    source = source * a_dev + lax.rem(row, a_dev)
    column = lax.broadcasted_iota(jnp.int32, (count, count), 1)
    chosen = (column == source).astype(jnp.float32).astype(jnp.bfloat16)
    amps = jnp.dot(chosen, held, preferred_element_type=jnp.float32).astype(jnp.bfloat16)
    odd = lax.rem(lax.broadcasted_iota(jnp.int32, (1, LANES), 1) // a_dev, 2) == 1
    rows = out_ref.shape[1]
    for q in range(b_count // 2):
        sums = []
        for b, step in ((2 * q, LANES - a_dev), (2 * q + 1, a_dev)):
            full = jnp.dot(amps, stack_ref[b], preferred_element_type=jnp.float32)
            mixed = jnp.where(odd, full[i_count:], full[:i_count])
            sums.append(mixed + pltpu.roll(mixed, step, 1))
        found = jnp.where(odd, sums[1], sums[0]).astype(out_ref.dtype)
        for k in range(out_ref.shape[0]):
            out_ref[k, :, q * LANES : (q + 1) * LANES] = found[k * rows : (k + 1) * rows]


def in_vmem(count):
    return [pl.BlockSpec(memory_space=pltpu.VMEM)] * count


def ladder_partials(place, near, far, quarters, b_count, i_count, con_count):
    right = (len(quarters) * quarters[0].shape[0], quarters[0].shape[1])
    depth = (near.shape[1] // b_count - 2) * (right[0] // b_count)
    pairs = 2 * near.size * right[0]
    return pl.pallas_call(
        ladder_kernel,
        out_shape=jax.ShapeDtypeStruct(
            (con_count, i_count // con_count, b_count * LANES // 2), jnp.bfloat16
        ),
        in_specs=[pl.BlockSpec(memory_space=pltpu.SMEM)] + in_vmem(2 + len(quarters)),
        out_specs=pl.BlockSpec(memory_space=pltpu.VMEM),
        scratch_shapes=[
            pltpu.VMEM((b_count, depth, LANES), jnp.bfloat16),
            pltpu.VMEM(right, jnp.bfloat16),
        ],
        compiler_params=pltpu.CompilerParams(vmem_limit_bytes=12 * 1024 * 1024),
        cost_estimate=pl.CostEstimate(
            flops=2 * pairs, bytes_accessed=4 * near.size, transcendentals=0
        ),
    )(place, near, far, *quarters)


def pack_kernel(rows_ref, amps_ref, other_ref, out_ref):
    count, cells = rows_ref.shape[0], amps_ref.shape[1] // 2
    for n in range(out_ref.shape[0]):
        out_ref[n, :count, :] = rows_ref[...]
    out_ref[:, count:, cells:] = jnp.zeros_like(out_ref[:, count:, cells:])
    for m, ref in enumerate((amps_ref, other_ref)):
        block = jnp.concatenate([ref[:, :cells], ref[:, cells:]], axis=0)
        for n in range(out_ref.shape[0]):
            first = count + m * block.shape[0]
            out_ref[n, first : first + block.shape[0], :cells] = block


def packed_copies(rows, amps, other, copies):
    count = rows.shape[0] + 4 * amps.shape[0]
    return pl.pallas_call(
        pack_kernel,
        out_shape=jax.ShapeDtypeStruct((copies, count, rows.shape[1]), rows.dtype),
        in_specs=in_vmem(3),
        out_specs=pl.BlockSpec(memory_space=pltpu.VMEM),
        compiler_params=pltpu.CompilerParams(vmem_limit_bytes=6 * 1024 * 1024),
        cost_estimate=pl.CostEstimate(
            flops=rows.size, bytes_accessed=16 * rows.size, transcendentals=0
        ),
    )(rows, amps, other)


def total_kernel(parts_ref, out_ref):
    total = parts_ref[0].astype(jnp.float32)
    for k in range(1, parts_ref.shape[0]):
        total = total + parts_ref[k].astype(jnp.float32)
    total = total.astype(out_ref.dtype)
    for o in range(out_ref.shape[0]):
        out_ref[o] = total


def totals(parts, copies):
    return pl.pallas_call(
        total_kernel,
        out_shape=jax.ShapeDtypeStruct((copies, *parts.shape[1:]), parts.dtype),
        in_specs=in_vmem(1),
        out_specs=pl.BlockSpec(memory_space=pltpu.VMEM),
        compiler_params=pltpu.CompilerParams(vmem_limit_bytes=4 * 1024 * 1024),
        cost_estimate=pl.CostEstimate(
            flops=parts.size, bytes_accessed=4 * parts.size, transcendentals=0
        ),
    )(parts)


def residual_kernel(ring, pairs_ref, swap_ref, every_ref, out_ref):
    slots, occ, width = out_ref.shape
    group = LANES // ring
    chunks = every_ref.shape[2] // LANES // 2
    lane_group = lax.broadcasted_iota(jnp.int32, (1, LANES), 1) // group

    def half_tile(a_tile, b_tile, c):
        holder = (a_tile // ring * ring + lax.rem(b_tile, ring)) * 2 + c
        first = b_tile // ring * (chunks * LANES)
        found = jnp.zeros((occ, LANES), jnp.float32)
        for m in range(chunks):
            block = every_ref[holder, :, pl.ds(pl.multiple_of(first + m * LANES, LANES), LANES)]
            block = block.astype(jnp.float32)
            shift = lax.rem((m + ring - lax.rem(a_tile, ring)) * group, LANES)
            found = jnp.where(lane_group == m, pltpu.roll(block, shift, 1), found)
        return found

    def tiles(role):
        return jnp.concatenate(
            [
                jnp.concatenate(
                    [half_tile(pairs_ref[s, role], pairs_ref[s, 1 - role], c) for c in range(2)],
                    axis=1,
                )
                for s in range(slots)
            ],
            axis=0,
        ).astype(jnp.bfloat16)

    def placed(rows, spot):
        column = lax.broadcasted_iota(jnp.int32, (width, width), 1)
        chosen = (column == spot).astype(jnp.float32).astype(jnp.bfloat16)
        return jnp.dot(rows, chosen, preferred_element_type=jnp.float32)

    lane = lax.broadcasted_iota(jnp.int32, (width, width), 0)
    core_b = lane // LANES
    core_a = lax.rem(lane // (group // 2) + core_b, 2)
    a = core_a * (TS // 2) + lax.rem(lane, TS // 2)
    b = core_b * (TS // 2) + lax.rem(lane, LANES) // group * 2 + lax.rem(lane // (TS // 2), 2)
    straight = placed(tiles(0), a * TS + b)
    row = lax.broadcasted_iota(jnp.int32, (slots * occ, slots * occ), 0)
    column = lax.broadcasted_iota(jnp.int32, (slots * occ, slots * occ), 1)
    source = row // occ * occ
    for i in range(occ):
        source = source + jnp.where(lax.rem(row, occ) == i, swap_ref[i], 0)
    chosen = (column == source).astype(jnp.float32).astype(jnp.bfloat16)
    swapped = jnp.dot(chosen, tiles(1), preferred_element_type=jnp.float32).astype(jnp.bfloat16)
    total = straight + placed(swapped, b * TS + a)
    for s in range(slots):
        out_ref[s] = total[s * occ : (s + 1) * occ]


def residual_tiles(pairs, swap, every, ring):
    slots, occ = pairs.shape[0], swap.shape[0]
    return pl.pallas_call(
        functools.partial(residual_kernel, ring),
        out_shape=jax.ShapeDtypeStruct((slots, occ, TS * TS), jnp.float32),
        in_specs=[pl.BlockSpec(memory_space=pltpu.SMEM)] * 2 + in_vmem(1),
        out_specs=pl.BlockSpec(memory_space=pltpu.VMEM),
        compiler_params=pltpu.CompilerParams(vmem_limit_bytes=8 * 1024 * 1024),
        cost_estimate=pl.CostEstimate(
            flops=100 * every.size, bytes_accessed=4 * every.size, transcendentals=0
        ),
    )(pairs, swap, every)


def on_device(chol, amplitudes, tile_pairs, partner, pair_swap):
    out_count = lax.axis_size(OUT)
    con_count = lax.axis_size(CONTRACT)
    ring = lax.axis_size("x")
    a_dev, c_dev, p_size = chol.shape
    i_count = amplitudes.shape[0] * out_count
    half = c_dev // 2

    other_amps = lax.ppermute(amplitudes, "yh", PAIR)
    rows = jnp.transpose(chol.reshape(a_dev, 2, half, p_size), (2, 1, 0, 3))
    packed = packed_copies(rows.reshape(-1, p_size), amplitudes, other_amps, ring)
    near = exchange(packed, "x")

    z, yl, yh = lax.axis_index("z"), lax.axis_index("yl"), lax.axis_index("yh")
    depth_z = lax.axis_size("z")
    window = chol.reshape(2, -1, p_size)
    piece = jnp.where(yl == 0, window[0], lax.ppermute(window[1], CONTRACT, [(0, 1)]))
    got = sum(lax.ppermute(piece, "z", [hop]) for hop in LONG)
    piece = jnp.where(z == 0, piece, got)
    got = lax.ppermute(piece, "z", MIDDLE)
    piece = jnp.where(functools.reduce(jnp.logical_or, [z == to for _, to in MIDDLE]), got, piece)
    reach = {}
    for to in range(depth_z):
        if to not in HOLDERS:
            steps = [((to - at + depth_z // 2) % depth_z - depth_z // 2, at) for at in SENDERS]
            step, at = min(steps, key=lambda pair: abs(pair[0]))
            reach.setdefault(step, []).append((at, to))
    steps = sorted(reach, key=abs, reverse=True)
    got = lax.ppermute(piece, "z", reach[steps[0]])
    got = sum((lax.ppermute(piece, "z", reach[step]) for step in steps[1:]), got)
    holder = functools.reduce(jnp.logical_or, [z == at for at in HOLDERS])
    piece = jnp.where(holder, piece, got)
    quarters = [piece] + [
        lax.ppermute(piece, ("yl", "yh"), [(at, at ^ q) for at in range(4)]) for q in (2, 1, 3)
    ]

    far = lax.ppermute(near, "core", PAIR)
    place = jnp.stack([lax.axis_index("core"), yh, 2 * yh + yl])
    partial = ladder_partials(place, near, far, quarters, 2 * a_dev, i_count, con_count)
    every = exchange(totals(exchange(partial, CONTRACT), out_count), OUT)

    slot_count, occ_dev = tile_pairs.shape[0] // out_count, i_count // con_count
    first = lax.axis_index(OUT) * slot_count
    pairs = lax.dynamic_slice_in_dim(tile_pairs, first, slot_count, 0)
    first = lax.axis_index(CONTRACT) * occ_dev
    swap = lax.dynamic_slice_in_dim(pair_swap, first, occ_dev, 0) - first
    return residual_tiles(pairs, swap, every, ring)


def solution(mesh):
    torus = Mesh(mesh.devices.reshape(16, 2, 2, 4, 2), ("z", "yl", "yh", "x", "core"))
    in_specs = (P(OUT, CONTRACT, None), P(OUT, CONTRACT), P(), P(), P())
    out_specs = P(OUT, CONTRACT, None)

    return jax.shard_map(
        on_device, mesh=torus, in_specs=in_specs, out_specs=out_specs, check_vma=False
    )
```

```python
import functools

import jax
import jax.numpy as jnp
from jax import lax
from jax.experimental import pallas as pl
from jax.experimental.pallas import tpu as pltpu
from jax.sharding import Mesh
from jax.sharding import PartitionSpec as P

TS = 16
LANES = 128
CONTRACT = ("z", "yl")
OUT = ("yh", "x", "core")
PAIR = [(0, 1), (1, 0)]
LONG, MIDDLE = [(0, 3), (0, 12)], [(3, 6), (12, 9), (0, 14)]
SENDERS, HOLDERS = (0, 3, 6, 9, 12), (0, 3, 6, 9, 12, 14)


def exchange(array, axes):
    return lax.all_to_all(array, axes, 0, 0, tiled=True)


def sent_to_all(array, axes):
    count = lax.axis_size(axes)
    return exchange(jnp.broadcast_to(array[None], (count, *array.shape)), axes)


def ladder_kernel(place_ref, near_ref, far_ref, amps_ref, right_ref, out_ref, stack_ref):
    b_count, depth, _ = stack_ref.shape
    ring, pair_rows = near_ref.shape[0], b_count
    c_pairs = near_ref.shape[1] // pair_rows
    a_dev = pair_rows // 2
    order = [lax.rem(place_ref[0] + ring - x, ring) for x in range(ring)]
    d_count = right_ref.shape[0] // b_count
    right = right_ref[...]
    for n in range(0, c_pairs, 2):
        left = jnp.concatenate(
            [
                ref[order[x], m * pair_rows : (m + 1) * pair_rows, :]
                for m in (n, n + 1)
                for x in range(ring)
                for ref in (near_ref, far_ref)
            ],
            axis=0,
        )
        part = lax.dot_general(
            right, left, (((1,), (1,)), ((), ())), preferred_element_type=jnp.float32
        ).astype(jnp.bfloat16)
        part = part.reshape(b_count, d_count, 2 * LANES)
        for h in range(2):
            rows = (n + h) * d_count
            stack_ref[:, rows : rows + d_count, :] = part[:, :, h * LANES : (h + 1) * LANES]
    i_count = amps_ref.shape[0]
    amps = jnp.concatenate([amps_ref[:, :depth], amps_ref[:, depth:]], axis=0)
    odd = lax.rem(lax.broadcasted_iota(jnp.int32, (1, LANES), 1) // a_dev, 2) == 1
    rows = out_ref.shape[1]
    for q in range(b_count // 2):
        sums = []
        for b, step in ((2 * q, LANES - a_dev), (2 * q + 1, a_dev)):
            full = jnp.dot(amps, stack_ref[b], preferred_element_type=jnp.float32)
            mixed = jnp.where(odd, full[i_count:], full[:i_count])
            sums.append(mixed + pltpu.roll(mixed, step, 1))
        found = jnp.where(odd, sums[1], sums[0]).astype(out_ref.dtype)
        for k in range(out_ref.shape[0]):
            out_ref[k, :, q * LANES : (q + 1) * LANES] = found[k * rows : (k + 1) * rows]


def in_vmem(count):
    return [pl.BlockSpec(memory_space=pltpu.VMEM)] * count


def ladder_partials(place, near, far, amps, right, b_count, con_count):
    i_count = amps.shape[0]
    pairs = 2 * near.size * right.shape[0]
    return pl.pallas_call(
        ladder_kernel,
        out_shape=jax.ShapeDtypeStruct(
            (con_count, i_count // con_count, b_count * LANES // 2), jnp.bfloat16
        ),
        in_specs=[pl.BlockSpec(memory_space=pltpu.SMEM)] + in_vmem(4),
        out_specs=pl.BlockSpec(memory_space=pltpu.VMEM),
        scratch_shapes=[pltpu.VMEM((b_count, amps.shape[1] // 2, LANES), jnp.bfloat16)],
        compiler_params=pltpu.CompilerParams(vmem_limit_bytes=12 * 1024 * 1024),
        cost_estimate=pl.CostEstimate(
            flops=2 * pairs, bytes_accessed=4 * near.size, transcendentals=0
        ),
    )(place, near, far, amps, right)


def total_kernel(parts_ref, out_ref):
    total = parts_ref[0].astype(jnp.float32)
    for k in range(1, parts_ref.shape[0]):
        total = total + parts_ref[k].astype(jnp.float32)
    total = total.astype(out_ref.dtype)
    for o in range(out_ref.shape[0]):
        out_ref[o] = total


def totals(parts, copies):
    return pl.pallas_call(
        total_kernel,
        out_shape=jax.ShapeDtypeStruct((copies, *parts.shape[1:]), parts.dtype),
        in_specs=in_vmem(1),
        out_specs=pl.BlockSpec(memory_space=pltpu.VMEM),
        compiler_params=pltpu.CompilerParams(vmem_limit_bytes=4 * 1024 * 1024),
        cost_estimate=pl.CostEstimate(
            flops=parts.size, bytes_accessed=4 * parts.size, transcendentals=0
        ),
    )(parts)


def residual_kernel(ring, pairs_ref, swap_ref, every_ref, out_ref):
    slots, occ, width = out_ref.shape
    group = LANES // ring
    chunks = every_ref.shape[2] // LANES // 2
    lane_group = lax.broadcasted_iota(jnp.int32, (1, LANES), 1) // group

    def half_tile(a_tile, b_tile, c):
        holder = (a_tile // ring * ring + lax.rem(b_tile, ring)) * 2 + c
        first = b_tile // ring * (chunks * LANES)
        found = jnp.zeros((occ, LANES), jnp.float32)
        for m in range(chunks):
            block = every_ref[holder, :, pl.ds(pl.multiple_of(first + m * LANES, LANES), LANES)]
            block = block.astype(jnp.float32)
            shift = lax.rem((m + ring - lax.rem(a_tile, ring)) * group, LANES)
            found = jnp.where(lane_group == m, pltpu.roll(block, shift, 1), found)
        return found

    def tiles(role):
        return jnp.concatenate(
            [
                jnp.concatenate(
                    [half_tile(pairs_ref[s, role], pairs_ref[s, 1 - role], c) for c in range(2)],
                    axis=1,
                )
                for s in range(slots)
            ],
            axis=0,
        ).astype(jnp.bfloat16)

    def placed(rows, spot):
        column = lax.broadcasted_iota(jnp.int32, (width, width), 1)
        chosen = (column == spot).astype(jnp.float32).astype(jnp.bfloat16)
        return jnp.dot(rows, chosen, preferred_element_type=jnp.float32)

    lane = lax.broadcasted_iota(jnp.int32, (width, width), 0)
    core_b = lane // LANES
    core_a = lax.rem(lane // (group // 2) + core_b, 2)
    a = core_a * (TS // 2) + lax.rem(lane, TS // 2)
    b = core_b * (TS // 2) + lax.rem(lane, LANES) // group * 2 + lax.rem(lane // (TS // 2), 2)
    straight = placed(tiles(0), a * TS + b)
    row = lax.broadcasted_iota(jnp.int32, (slots * occ, slots * occ), 0)
    column = lax.broadcasted_iota(jnp.int32, (slots * occ, slots * occ), 1)
    source = row // occ * occ
    for i in range(occ):
        source = source + jnp.where(lax.rem(row, occ) == i, swap_ref[i], 0)
    chosen = (column == source).astype(jnp.float32).astype(jnp.bfloat16)
    swapped = jnp.dot(chosen, tiles(1), preferred_element_type=jnp.float32).astype(jnp.bfloat16)
    total = straight + placed(swapped, b * TS + a)
    for s in range(slots):
        out_ref[s] = total[s * occ : (s + 1) * occ]


def residual_tiles(pairs, swap, every, ring):
    slots, occ = pairs.shape[0], swap.shape[0]
    return pl.pallas_call(
        functools.partial(residual_kernel, ring),
        out_shape=jax.ShapeDtypeStruct((slots, occ, TS * TS), jnp.float32),
        in_specs=[pl.BlockSpec(memory_space=pltpu.SMEM)] * 2 + in_vmem(1),
        out_specs=pl.BlockSpec(memory_space=pltpu.VMEM),
        compiler_params=pltpu.CompilerParams(vmem_limit_bytes=8 * 1024 * 1024),
        cost_estimate=pl.CostEstimate(
            flops=100 * every.size, bytes_accessed=4 * every.size, transcendentals=0
        ),
    )(pairs, swap, every)


def on_device(chol, amplitudes, tile_pairs, partner, pair_swap):
    out_count = lax.axis_size(OUT)
    con_count = lax.axis_size(CONTRACT)
    ring = lax.axis_size("x")
    a_dev, c_dev, p_size = chol.shape
    i_count = amplitudes.shape[0] * out_count
    half = c_dev // 2

    rows = jnp.transpose(chol.reshape(a_dev, 2, half, p_size), (2, 1, 0, 3))
    rows = rows.reshape(-1, p_size)
    near = [rows] + [
        lax.ppermute(rows, "x", [(x, (x + shift) % ring) for x in range(ring)])
        for shift in range(1, ring)
    ]
    amps = sent_to_all(amplitudes, OUT).reshape(i_count, -1)

    z, yl = lax.axis_index("z"), lax.axis_index("yl")
    depth_z = lax.axis_size("z")
    window = chol.reshape(2, -1, p_size)
    piece = jnp.where(yl == 0, window[0], lax.ppermute(window[1], CONTRACT, [(0, 1)]))
    got = sum(lax.ppermute(piece, "z", [hop]) for hop in LONG)
    piece = jnp.where(z == 0, piece, got)
    got = lax.ppermute(piece, "z", MIDDLE)
    piece = jnp.where(functools.reduce(jnp.logical_or, [z == to for _, to in MIDDLE]), got, piece)
    reach = {}
    for to in range(depth_z):
        if to not in HOLDERS:
            steps = [((to - at + depth_z // 2) % depth_z - depth_z // 2, at) for at in SENDERS]
            step, at = min(steps, key=lambda pair: abs(pair[0]))
            reach.setdefault(step, []).append((at, to))
    steps = sorted(reach, key=abs, reverse=True)
    got = lax.ppermute(piece, "z", reach[steps[0]])
    got = sum((lax.ppermute(piece, "z", reach[step]) for step in steps[1:]), got)
    holder = functools.reduce(jnp.logical_or, [z == at for at in HOLDERS])
    piece = jnp.where(holder, piece, got)
    right = sent_to_all(piece, ("yh", "yl")).reshape(-1, p_size)

    near = jnp.stack(near, axis=0)
    far = lax.ppermute(near, "core", PAIR)

    place = lax.axis_index("x").reshape(1)
    partial = ladder_partials(place, near, far, amps, right, 2 * a_dev, con_count)
    every = exchange(totals(exchange(partial, CONTRACT), out_count), OUT)

    slot_count, occ_dev = tile_pairs.shape[0] // out_count, i_count // con_count
    first = lax.axis_index(OUT) * slot_count
    pairs = lax.dynamic_slice_in_dim(tile_pairs, first, slot_count, 0)
    first = lax.axis_index(CONTRACT) * occ_dev
    swap = lax.dynamic_slice_in_dim(pair_swap, first, occ_dev, 0) - first
    return residual_tiles(pairs, swap, every, ring)


def solution(mesh):
    torus = Mesh(mesh.devices.reshape(16, 2, 2, 4, 2), ("z", "yl", "yh", "x", "core"))
    in_specs = (P(OUT, CONTRACT, None), P(OUT, CONTRACT), P(), P(), P())
    out_specs = P(OUT, CONTRACT, None)

    return jax.shard_map(
        on_device, mesh=torus, in_specs=in_specs, out_specs=out_specs, check_vma=False
    )
```

```python
import functools

import jax
import jax.numpy as jnp
from jax import lax
from jax.experimental import pallas as pl
from jax.experimental.pallas import tpu as pltpu
from jax.sharding import Mesh
from jax.sharding import PartitionSpec as P

TS = 16
LANES = 128
CONTRACT = ("z", "yl")
OUT = ("yh", "x", "core")
PAIR = [(0, 1), (1, 0)]
LONG, MIDDLE = [(0, 3), (0, 13)], [(3, 6), (13, 10)]
SENDERS = (0, 3, 6, 10, 13)


def exchange(array, axes):
    return lax.all_to_all(array, axes, 0, 0, tiled=True)


def ladder_kernel(place_ref, near_ref, far_ref, *refs):
    *quarter_refs, last_ref, out_ref, stack_ref, right_ref, amps_ref, landing_ref, landed = refs
    core, yh, own = place_ref[0], place_ref[1], place_ref[2]
    landing = pltpu.make_async_copy(last_ref, landing_ref, landed)
    landing.start()
    b_count, depth, _ = stack_ref.shape
    ring, pair_rows = near_ref.shape[0], b_count
    c_pairs = near_ref.shape[1] // pair_rows - 2
    a_dev = pair_rows // 2
    d_count = right_ref.shape[0] // b_count
    for m in range(2):
        for rc, ref in enumerate((near_ref, far_ref)):
            for x in range(ring):
                place = (lax.rem(yh + m, 2) * ring + x) * 2 + lax.rem(core + rc, 2)
                first = (c_pairs + m) * pair_rows
                block = ref[x, first : first + pair_rows, :depth].astype(jnp.float32)
                for g in range(2):
                    amps_ref[g, place] = block[g * a_dev : (g + 1) * a_dev]
    landing.wait()
    size = landing_ref.shape[0]
    for q, ref in enumerate((*quarter_refs, landing_ref)):
        right_ref[pl.ds(pl.multiple_of((own ^ q) * size, size), size), :] = ref[...]
    right = right_ref[...]
    for n in range(0, c_pairs, 2):
        left = jnp.concatenate(
            [
                ref[x, m * pair_rows : (m + 1) * pair_rows, :]
                for m in (n, n + 1)
                for x in range(ring)
                for ref in (near_ref, far_ref)
            ],
            axis=0,
        )
        part = lax.dot_general(
            right, left, (((1,), (1,)), ((), ())), preferred_element_type=jnp.float32
        ).astype(jnp.bfloat16)
        part = part.reshape(b_count, d_count, 2 * LANES)
        for h in range(2):
            rows = (n + h) * d_count
            stack_ref[:, rows : rows + d_count, :] = part[:, :, h * LANES : (h + 1) * LANES]
    i_count = amps_ref.shape[1] * a_dev
    amps = amps_ref[...].reshape(2 * i_count, depth).astype(jnp.bfloat16)
    odd = lax.rem(lax.broadcasted_iota(jnp.int32, (1, LANES), 1) // a_dev, 2) == 1
    rows = out_ref.shape[1]
    for q in range(b_count // 2):
        sums = []
        for b, step in ((2 * q, LANES - a_dev), (2 * q + 1, a_dev)):
            full = jnp.dot(amps, stack_ref[b], preferred_element_type=jnp.float32)
            mixed = jnp.where(odd, full[i_count:], full[:i_count])
            sums.append(mixed + pltpu.roll(mixed, step, 1))
        found = jnp.where(odd, sums[1], sums[0]).astype(out_ref.dtype)
        for k in range(out_ref.shape[0]):
            out_ref[k, :, q * LANES : (q + 1) * LANES] = found[k * rows : (k + 1) * rows]


def in_vmem(count):
    return [pl.BlockSpec(memory_space=pltpu.VMEM)] * count


def ladder_partials(place, near, far, quarters, b_count, i_count, con_count):
    right = (len(quarters) * quarters[0].shape[0], quarters[0].shape[1])
    depth = (near.shape[1] // b_count - 2) * (right[0] // b_count)
    pairs = 2 * near.size * right[0]
    return pl.pallas_call(
        ladder_kernel,
        out_shape=jax.ShapeDtypeStruct(
            (con_count, i_count // con_count, b_count * LANES // 2), jnp.bfloat16
        ),
        in_specs=[pl.BlockSpec(memory_space=pltpu.SMEM)] + in_vmem(1 + len(quarters))
        + [pl.BlockSpec(memory_space=pl.ANY)],
        out_specs=pl.BlockSpec(memory_space=pltpu.VMEM),
        scratch_shapes=[
            pltpu.VMEM((b_count, depth, LANES), jnp.bfloat16),
            pltpu.VMEM(right, jnp.bfloat16),
            pltpu.VMEM((2, 4 * near.shape[0], b_count // 2, depth), jnp.float32),
            pltpu.VMEM(quarters[-1].shape, jnp.bfloat16),
            pltpu.SemaphoreType.DMA,
        ],
        compiler_params=pltpu.CompilerParams(vmem_limit_bytes=12 * 1024 * 1024),
        cost_estimate=pl.CostEstimate(
            flops=2 * pairs, bytes_accessed=4 * near.size, transcendentals=0
        ),
    )(place, near, far, *quarters)


def pack_kernel(rows_ref, amps_ref, other_ref, out_ref):
    count, cells = rows_ref.shape[0], amps_ref.shape[1] // 2
    for n in range(out_ref.shape[0]):
        out_ref[n, :count, :] = rows_ref[...]
    out_ref[:, count:, cells:] = jnp.zeros_like(out_ref[:, count:, cells:])
    for m, ref in enumerate((amps_ref, other_ref)):
        block = jnp.concatenate([ref[:, :cells], ref[:, cells:]], axis=0)
        for n in range(out_ref.shape[0]):
            first = count + m * block.shape[0]
            out_ref[n, first : first + block.shape[0], :cells] = block


def packed_copies(rows, amps, other, copies):
    count = rows.shape[0] + 4 * amps.shape[0]
    return pl.pallas_call(
        pack_kernel,
        out_shape=jax.ShapeDtypeStruct((copies, count, rows.shape[1]), rows.dtype),
        in_specs=in_vmem(3),
        out_specs=pl.BlockSpec(memory_space=pltpu.VMEM),
        compiler_params=pltpu.CompilerParams(vmem_limit_bytes=6 * 1024 * 1024),
        cost_estimate=pl.CostEstimate(
            flops=rows.size, bytes_accessed=16 * rows.size, transcendentals=0
        ),
    )(rows, amps, other)


def total_kernel(parts_ref, out_ref):
    total = parts_ref[0].astype(jnp.float32)
    for k in range(1, parts_ref.shape[0]):
        total = total + parts_ref[k].astype(jnp.float32)
    total = total.astype(out_ref.dtype)
    for o in range(out_ref.shape[0]):
        out_ref[o] = total


def totals(parts, copies):
    return pl.pallas_call(
        total_kernel,
        out_shape=jax.ShapeDtypeStruct((copies, *parts.shape[1:]), parts.dtype),
        in_specs=in_vmem(1),
        out_specs=pl.BlockSpec(memory_space=pltpu.VMEM),
        compiler_params=pltpu.CompilerParams(vmem_limit_bytes=4 * 1024 * 1024),
        cost_estimate=pl.CostEstimate(
            flops=parts.size, bytes_accessed=4 * parts.size, transcendentals=0
        ),
    )(parts)


def residual_kernel(ring, pairs_ref, swap_ref, every_ref, out_ref):
    slots, occ, width = out_ref.shape
    group = LANES // ring
    chunks = every_ref.shape[2] // LANES // 2
    lane_group = lax.broadcasted_iota(jnp.int32, (1, LANES), 1) // group

    def half_tile(a_tile, b_tile, c):
        holder = (a_tile // ring * ring + lax.rem(b_tile, ring)) * 2 + c
        first = b_tile // ring * (chunks * LANES)
        found = jnp.zeros((occ, LANES), jnp.float32)
        for m in range(chunks):
            block = every_ref[holder, :, pl.ds(pl.multiple_of(first + m * LANES, LANES), LANES)]
            block = block.astype(jnp.float32)
            shift = lax.rem((m + ring - lax.rem(a_tile, ring)) * group, LANES)
            found = jnp.where(lane_group == m, pltpu.roll(block, shift, 1), found)
        return found

    def tiles(role):
        return jnp.concatenate(
            [
                jnp.concatenate(
                    [half_tile(pairs_ref[s, role], pairs_ref[s, 1 - role], c) for c in range(2)],
                    axis=1,
                )
                for s in range(slots)
            ],
            axis=0,
        ).astype(jnp.bfloat16)

    def placed(rows, spot):
        column = lax.broadcasted_iota(jnp.int32, (width, width), 1)
        chosen = (column == spot).astype(jnp.float32).astype(jnp.bfloat16)
        return jnp.dot(rows, chosen, preferred_element_type=jnp.float32)

    lane = lax.broadcasted_iota(jnp.int32, (width, width), 0)
    core_b = lane // LANES
    core_a = lax.rem(lane // (group // 2) + core_b, 2)
    a = core_a * (TS // 2) + lax.rem(lane, TS // 2)
    b = core_b * (TS // 2) + lax.rem(lane, LANES) // group * 2 + lax.rem(lane // (TS // 2), 2)
    straight = placed(tiles(0), a * TS + b)
    row = lax.broadcasted_iota(jnp.int32, (slots * occ, slots * occ), 0)
    column = lax.broadcasted_iota(jnp.int32, (slots * occ, slots * occ), 1)
    source = row // occ * occ
    for i in range(occ):
        source = source + jnp.where(lax.rem(row, occ) == i, swap_ref[i], 0)
    chosen = (column == source).astype(jnp.float32).astype(jnp.bfloat16)
    swapped = jnp.dot(chosen, tiles(1), preferred_element_type=jnp.float32).astype(jnp.bfloat16)
    total = straight + placed(swapped, b * TS + a)
    for s in range(slots):
        out_ref[s] = total[s * occ : (s + 1) * occ]


def residual_tiles(pairs, swap, every, ring):
    slots, occ = pairs.shape[0], swap.shape[0]
    return pl.pallas_call(
        functools.partial(residual_kernel, ring),
        out_shape=jax.ShapeDtypeStruct((slots, occ, TS * TS), jnp.float32),
        in_specs=[pl.BlockSpec(memory_space=pltpu.SMEM)] * 2 + in_vmem(1),
        out_specs=pl.BlockSpec(memory_space=pltpu.VMEM),
        compiler_params=pltpu.CompilerParams(vmem_limit_bytes=8 * 1024 * 1024),
        cost_estimate=pl.CostEstimate(
            flops=100 * every.size, bytes_accessed=4 * every.size, transcendentals=0
        ),
    )(pairs, swap, every)


def on_device(chol, amplitudes, tile_pairs, partner, pair_swap):
    out_count = lax.axis_size(OUT)
    con_count = lax.axis_size(CONTRACT)
    ring = lax.axis_size("x")
    a_dev, c_dev, p_size = chol.shape
    i_count = amplitudes.shape[0] * out_count
    half = c_dev // 2

    other_amps = lax.ppermute(amplitudes, "yh", PAIR)
    rows = jnp.transpose(chol.reshape(a_dev, 2, half, p_size), (2, 1, 0, 3))
    packed = packed_copies(rows.reshape(-1, p_size), amplitudes, other_amps, ring)
    near = exchange(packed, "x")

    z, yl, yh = lax.axis_index("z"), lax.axis_index("yl"), lax.axis_index("yh")
    depth_z = lax.axis_size("z")
    window = chol.reshape(2, -1, p_size)
    piece = jnp.where(yl == 0, window[0], lax.ppermute(window[1], CONTRACT, [(0, 1)]))
    got = sum(lax.ppermute(piece, "z", [hop]) for hop in LONG)
    piece = jnp.where(z == 0, piece, got)
    got = lax.ppermute(piece, "z", MIDDLE)
    piece = jnp.where(functools.reduce(jnp.logical_or, [z == to for _, to in MIDDLE]), got, piece)
    reach = {}
    for to in range(depth_z):
        if to not in SENDERS:
            steps = [((to - at + depth_z // 2) % depth_z - depth_z // 2, at) for at in SENDERS]
            step, at = min(steps, key=lambda pair: abs(pair[0]))
            reach.setdefault(step, []).append((at, to))
    steps = sorted(reach, key=abs, reverse=True)
    got = lax.ppermute(piece, "z", reach[steps[0]])
    got = sum((lax.ppermute(piece, "z", reach[step]) for step in steps[1:]), got)
    sender = functools.reduce(jnp.logical_or, [z == at for at in SENDERS])
    piece = jnp.where(sender, piece, got)
    quarters = [piece] + [
        lax.ppermute(piece, ("yl", "yh"), [(at, at ^ q) for at in range(4)]) for q in (2, 1, 3)
    ]

    far = lax.ppermute(near, "core", PAIR)
    slot_count, occ_dev = tile_pairs.shape[0] // out_count, i_count // con_count
    first = lax.axis_index(OUT) * slot_count
    pairs = lax.dynamic_slice_in_dim(tile_pairs, first, slot_count, 0)
    first = lax.axis_index(CONTRACT) * occ_dev
    swap = lax.dynamic_slice_in_dim(pair_swap, first, occ_dev, 0) - first
    far, pairs, swap = lax.optimization_barrier((far, pairs, swap))
    place = jnp.stack([lax.axis_index("core"), yh, 2 * yh + yl])
    partial = ladder_partials(place, near, far, quarters, 2 * a_dev, i_count, con_count)
    every = exchange(totals(exchange(partial, CONTRACT), out_count), OUT)

    return residual_tiles(pairs, swap, every, ring)


def solution(mesh):
    torus = Mesh(mesh.devices.reshape(16, 2, 2, 4, 2), ("z", "yl", "yh", "x", "core"))
    in_specs = (P(OUT, CONTRACT, None), P(OUT, CONTRACT), P(), P(), P())
    out_specs = P(OUT, CONTRACT, None)

    return jax.shard_map(
        on_device, mesh=torus, in_specs=in_specs, out_specs=out_specs, check_vma=False
    )
```

```python
import functools

import jax
import jax.numpy as jnp
from jax import lax
from jax.experimental import pallas as pl
from jax.experimental.pallas import tpu as pltpu
from jax.sharding import Mesh
from jax.sharding import PartitionSpec as P

TS = 16
LANES = 128
CONTRACT = ("z", "yl")
OUT = ("yh", "x", "core")
PAIR = [(0, 1), (1, 0)]
LONG, MIDDLE = [(0, 3), (0, 13)], [(3, 6), (13, 10)]
SENDERS = (0, 3, 6, 10, 13)


def exchange(array, axes):
    return lax.all_to_all(array, axes, 0, 0, tiled=True)


def ladder_kernel(place_ref, near_ref, far_ref, *refs):
    *quarter_refs, last_ref, out_ref, stack_ref, right_ref, amps_ref, landing_ref, rows_ref, landed = refs
    core, yh, own = place_ref[0], place_ref[1], place_ref[2]
    landing = pltpu.make_async_copy(last_ref, landing_ref, landed)
    landing.start()
    b_count, depth, _ = stack_ref.shape
    ring, pair_rows = near_ref.shape[0], b_count
    c_pairs = near_ref.shape[1] // pair_rows - 2
    a_dev = pair_rows // 2
    d_count = right_ref.shape[0] // b_count
    for m in range(2):
        for rc, ref in enumerate((near_ref, far_ref)):
            for x in range(ring):
                place = (lax.rem(yh + m, 2) * ring + x) * 2 + lax.rem(core + rc, 2)
                first = (c_pairs + m) * pair_rows
                block = ref[x, first : first + pair_rows, :depth].astype(jnp.float32)
                for g in range(2):
                    amps_ref[g, place] = block[g * a_dev : (g + 1) * a_dev]
    i_count = amps_ref.shape[1] * a_dev
    rows_ref[...] = amps_ref[...].reshape(2 * i_count, depth).astype(rows_ref.dtype)
    landing.wait()
    size = landing_ref.shape[0]
    for q, ref in enumerate((*quarter_refs, landing_ref)):
        right_ref[pl.ds(pl.multiple_of((own ^ q) * size, size), size), :] = ref[...]
    for n in range(0, c_pairs, 2):
        left = jnp.concatenate(
            [
                ref[x, m * pair_rows : (m + 1) * pair_rows, :]
                for m in (n, n + 1)
                for x in range(ring)
                for ref in (near_ref, far_ref)
            ],
            axis=0,
        )
        part = lax.dot_general(
            right_ref[...], left, (((1,), (1,)), ((), ())), preferred_element_type=jnp.float32
        ).astype(jnp.bfloat16)
        part = part.reshape(b_count, d_count, 2 * LANES)
        for h in range(2):
            rows = (n + h) * d_count
            stack_ref[:, rows : rows + d_count, :] = part[:, :, h * LANES : (h + 1) * LANES]
    odd = lax.rem(lax.broadcasted_iota(jnp.int32, (1, LANES), 1) // a_dev, 2) == 1
    rows = out_ref.shape[1]
    for q in range(b_count // 2):
        sums = []
        for b, step in ((2 * q, LANES - a_dev), (2 * q + 1, a_dev)):
            full = jnp.dot(rows_ref[...], stack_ref[b], preferred_element_type=jnp.float32)
            mixed = jnp.where(odd, full[i_count:], full[:i_count])
            sums.append(mixed + pltpu.roll(mixed, step, 1))
        found = jnp.where(odd, sums[1], sums[0]).astype(out_ref.dtype)
        for k in range(out_ref.shape[0]):
            out_ref[k, :, q * LANES : (q + 1) * LANES] = found[k * rows : (k + 1) * rows]


def in_vmem(count):
    return [pl.BlockSpec(memory_space=pltpu.VMEM)] * count


def ladder_partials(place, near, far, quarters, b_count, i_count, con_count):
    right = (len(quarters) * quarters[0].shape[0], quarters[0].shape[1])
    depth = (near.shape[1] // b_count - 2) * (right[0] // b_count)
    pairs = 2 * near.size * right[0]
    return pl.pallas_call(
        ladder_kernel,
        out_shape=jax.ShapeDtypeStruct(
            (con_count, i_count // con_count, b_count * LANES // 2), jnp.bfloat16
        ),
        in_specs=[pl.BlockSpec(memory_space=pltpu.SMEM)] + in_vmem(1 + len(quarters))
        + [pl.BlockSpec(memory_space=pl.ANY)],
        out_specs=pl.BlockSpec(memory_space=pltpu.VMEM),
        scratch_shapes=[
            pltpu.VMEM((b_count, depth, LANES), jnp.bfloat16),
            pltpu.VMEM(right, jnp.bfloat16),
            pltpu.VMEM((2, 4 * near.shape[0], b_count // 2, depth), jnp.float32),
            pltpu.VMEM(quarters[-1].shape, jnp.bfloat16),
            pltpu.VMEM((2 * i_count, depth), jnp.bfloat16),
            pltpu.SemaphoreType.DMA,
        ],
        compiler_params=pltpu.CompilerParams(vmem_limit_bytes=12 * 1024 * 1024),
        cost_estimate=pl.CostEstimate(
            flops=2 * pairs, bytes_accessed=4 * near.size, transcendentals=0
        ),
    )(place, near, far, *quarters)


def pack_kernel(rows_ref, amps_ref, other_ref, out_ref):
    count, cells = rows_ref.shape[0], amps_ref.shape[1] // 2
    for n in range(out_ref.shape[0]):
        out_ref[n, :count, :] = rows_ref[...]
    out_ref[:, count:, cells:] = jnp.zeros_like(out_ref[:, count:, cells:])
    for m, ref in enumerate((amps_ref, other_ref)):
        block = jnp.concatenate([ref[:, :cells], ref[:, cells:]], axis=0)
        for n in range(out_ref.shape[0]):
            first = count + m * block.shape[0]
            out_ref[n, first : first + block.shape[0], :cells] = block


def packed_copies(rows, amps, other, copies):
    count = rows.shape[0] + 4 * amps.shape[0]
    return pl.pallas_call(
        pack_kernel,
        out_shape=jax.ShapeDtypeStruct((copies, count, rows.shape[1]), rows.dtype),
        in_specs=in_vmem(3),
        out_specs=pl.BlockSpec(memory_space=pltpu.VMEM),
        compiler_params=pltpu.CompilerParams(vmem_limit_bytes=6 * 1024 * 1024),
        cost_estimate=pl.CostEstimate(
            flops=rows.size, bytes_accessed=16 * rows.size, transcendentals=0
        ),
    )(rows, amps, other)


def total_kernel(parts_ref, out_ref):
    total = parts_ref[0].astype(jnp.float32)
    for k in range(1, parts_ref.shape[0]):
        total = total + parts_ref[k].astype(jnp.float32)
    total = total.astype(out_ref.dtype)
    for o in range(out_ref.shape[0]):
        out_ref[o] = total


def totals(parts, copies):
    return pl.pallas_call(
        total_kernel,
        out_shape=jax.ShapeDtypeStruct((copies, *parts.shape[1:]), parts.dtype),
        in_specs=in_vmem(1),
        out_specs=pl.BlockSpec(memory_space=pltpu.VMEM),
        compiler_params=pltpu.CompilerParams(vmem_limit_bytes=4 * 1024 * 1024),
        cost_estimate=pl.CostEstimate(
            flops=parts.size, bytes_accessed=4 * parts.size, transcendentals=0
        ),
    )(parts)


def residual_kernel(ring, pairs_ref, swap_ref, every_ref, out_ref):
    slots, occ, width = out_ref.shape
    group = LANES // ring
    chunks = every_ref.shape[2] // LANES // 2
    lane_group = lax.broadcasted_iota(jnp.int32, (1, LANES), 1) // group

    def half_tile(a_tile, b_tile, c):
        holder = (a_tile // ring * ring + lax.rem(b_tile, ring)) * 2 + c
        first = b_tile // ring * (chunks * LANES)
        found = jnp.zeros((occ, LANES), jnp.float32)
        for m in range(chunks):
            block = every_ref[holder, :, pl.ds(pl.multiple_of(first + m * LANES, LANES), LANES)]
            block = block.astype(jnp.float32)
            shift = lax.rem((m + ring - lax.rem(a_tile, ring)) * group, LANES)
            found = jnp.where(lane_group == m, pltpu.roll(block, shift, 1), found)
        return found

    def tiles(role):
        return jnp.concatenate(
            [
                jnp.concatenate(
                    [half_tile(pairs_ref[s, role], pairs_ref[s, 1 - role], c) for c in range(2)],
                    axis=1,
                )
                for s in range(slots)
            ],
            axis=0,
        ).astype(jnp.bfloat16)

    def placed(rows, spot):
        column = lax.broadcasted_iota(jnp.int32, (width, width), 1)
        chosen = (column == spot).astype(jnp.float32).astype(jnp.bfloat16)
        return jnp.dot(rows, chosen, preferred_element_type=jnp.float32)

    lane = lax.broadcasted_iota(jnp.int32, (width, width), 0)
    core_b = lane // LANES
    core_a = lax.rem(lane // (group // 2) + core_b, 2)
    a = core_a * (TS // 2) + lax.rem(lane, TS // 2)
    b = core_b * (TS // 2) + lax.rem(lane, LANES) // group * 2 + lax.rem(lane // (TS // 2), 2)
    straight = placed(tiles(0), a * TS + b)
    row = lax.broadcasted_iota(jnp.int32, (slots * occ, slots * occ), 0)
    column = lax.broadcasted_iota(jnp.int32, (slots * occ, slots * occ), 1)
    source = row // occ * occ
    for i in range(occ):
        source = source + jnp.where(lax.rem(row, occ) == i, swap_ref[i], 0)
    chosen = (column == source).astype(jnp.float32).astype(jnp.bfloat16)
    swapped = jnp.dot(chosen, tiles(1), preferred_element_type=jnp.float32).astype(jnp.bfloat16)
    total = straight + placed(swapped, b * TS + a)
    for s in range(slots):
        out_ref[s] = total[s * occ : (s + 1) * occ]


def residual_tiles(pairs, swap, every, ring):
    slots, occ = pairs.shape[0], swap.shape[0]
    return pl.pallas_call(
        functools.partial(residual_kernel, ring),
        out_shape=jax.ShapeDtypeStruct((slots, occ, TS * TS), jnp.float32),
        in_specs=[pl.BlockSpec(memory_space=pltpu.SMEM)] * 2 + in_vmem(1),
        out_specs=pl.BlockSpec(memory_space=pltpu.VMEM),
        compiler_params=pltpu.CompilerParams(vmem_limit_bytes=8 * 1024 * 1024),
        cost_estimate=pl.CostEstimate(
            flops=100 * every.size, bytes_accessed=4 * every.size, transcendentals=0
        ),
    )(pairs, swap, every)


def on_device(chol, amplitudes, tile_pairs, partner, pair_swap):
    out_count = lax.axis_size(OUT)
    con_count = lax.axis_size(CONTRACT)
    ring = lax.axis_size("x")
    a_dev, c_dev, p_size = chol.shape
    i_count = amplitudes.shape[0] * out_count
    half = c_dev // 2

    other_amps = lax.ppermute(amplitudes, "yh", PAIR)
    rows = jnp.transpose(chol.reshape(a_dev, 2, half, p_size), (2, 1, 0, 3))
    packed = packed_copies(rows.reshape(-1, p_size), amplitudes, other_amps, ring)
    near = exchange(packed, "x")

    z, yl, yh = lax.axis_index("z"), lax.axis_index("yl"), lax.axis_index("yh")
    depth_z = lax.axis_size("z")
    window = chol.reshape(2, -1, p_size)
    piece = jnp.where(yl == 0, window[0], lax.ppermute(window[1], CONTRACT, [(0, 1)]))
    got = sum(lax.ppermute(piece, "z", [hop]) for hop in LONG)
    piece = jnp.where(z == 0, piece, got)
    got = lax.ppermute(piece, "z", MIDDLE)
    piece = jnp.where(functools.reduce(jnp.logical_or, [z == to for _, to in MIDDLE]), got, piece)
    reach = {}
    for to in range(depth_z):
        if to not in SENDERS:
            steps = [((to - at + depth_z // 2) % depth_z - depth_z // 2, at) for at in SENDERS]
            step, at = min(steps, key=lambda pair: abs(pair[0]))
            reach.setdefault(step, []).append((at, to))
    steps = sorted(reach, key=abs, reverse=True)
    got = lax.ppermute(piece, "z", reach[steps[0]])
    got = sum((lax.ppermute(piece, "z", reach[step]) for step in steps[1:]), got)
    sender = functools.reduce(jnp.logical_or, [z == at for at in SENDERS])
    piece = jnp.where(sender, piece, got)
    quarters = [piece] + [
        lax.ppermute(piece, ("yl", "yh"), [(at, at ^ q) for at in range(4)]) for q in (2, 1, 3)
    ]

    far = lax.ppermute(near, "core", PAIR)
    slot_count, occ_dev = tile_pairs.shape[0] // out_count, i_count // con_count
    first = lax.axis_index(OUT) * slot_count
    pairs = lax.dynamic_slice_in_dim(tile_pairs, first, slot_count, 0)
    first = lax.axis_index(CONTRACT) * occ_dev
    swap = lax.dynamic_slice_in_dim(pair_swap, first, occ_dev, 0) - first
    far, pairs, swap = lax.optimization_barrier((far, pairs, swap))
    place = jnp.stack([lax.axis_index("core"), yh, 2 * yh + yl])
    partial = ladder_partials(place, near, far, quarters, 2 * a_dev, i_count, con_count)
    every = exchange(totals(exchange(partial, CONTRACT), out_count), OUT)

    return residual_tiles(pairs, swap, every, ring)


def solution(mesh):
    torus = Mesh(mesh.devices.reshape(16, 2, 2, 4, 2), ("z", "yl", "yh", "x", "core"))
    in_specs = (P(OUT, CONTRACT, None), P(OUT, CONTRACT), P(), P(), P())
    out_specs = P(OUT, CONTRACT, None)

    return jax.shard_map(
        on_device, mesh=torus, in_specs=in_specs, out_specs=out_specs, check_vma=False
    )
```

```python
import functools

import jax
import jax.numpy as jnp
from jax import lax
from jax.experimental import pallas as pl
from jax.experimental.pallas import tpu as pltpu
from jax.sharding import Mesh
from jax.sharding import PartitionSpec as P

TS = 16
LANES = 128
CONTRACT = ("z", "yl")
OUT = ("yh", "x", "core")
PAIR = [(0, 1), (1, 0)]
LONG, MIDDLE = [(0, 3), (0, 13)], [(3, 6), (13, 10)]
SENDERS = (0, 3, 6, 10, 13)


def exchange(array, axes):
    return lax.all_to_all(array, axes, 0, 0, tiled=True)


def ladder_kernel(place_ref, near_ref, far_ref, *refs):
    *quarter_refs, last_ref, out_ref, stack_ref, landing_ref, landed = refs
    core, yh, own = place_ref[0], place_ref[1], place_ref[2]
    landing = pltpu.make_async_copy(last_ref, landing_ref, landed)
    landing.start()
    quarter_refs = [*quarter_refs, landing_ref]
    b_count, depth, _ = stack_ref.shape
    ring, pair_rows = near_ref.shape[0], b_count
    c_pairs = near_ref.shape[1] // pair_rows - 2
    a_dev = pair_rows // 2
    some = b_count // len(quarter_refs)
    d_count = landing_ref.shape[0] // some
    odd = lax.rem(lax.broadcasted_iota(jnp.int32, (1, 1, LANES), 2) // a_dev, 2) == 1
    blocks = 4 * ring
    for first in range(0, len(quarter_refs), 2):
        if first + 2 == len(quarter_refs):
            landing.wait()
        for n in range(0, c_pairs, 2):
            left = jnp.concatenate(
                [
                    ref[x, m * pair_rows : (m + 1) * pair_rows, :]
                    for m in (n, n + 1)
                    for x in range(ring)
                    for ref in (near_ref, far_ref)
                ],
                axis=0,
            )
            right = jnp.concatenate([ref[...] for ref in quarter_refs[first : first + 2]], axis=0)
            part = lax.dot_general(
                right, left, (((1,), (1,)), ((), ())), preferred_element_type=jnp.float32
            ).astype(jnp.bfloat16)
            part = part.reshape(2 * some, d_count, 2 * LANES)
            for h in range(2):
                rows = (n + h) * d_count
                stack_ref[first * some : (first + 2) * some, rows : rows + d_count, :] = part[
                    :, :, h * LANES : (h + 1) * LANES
                ]
        for q in range(first * some // 2, (first + 2) * some // 2):
            amps = jnp.concatenate(
                [
                    ref[x, m * pair_rows : (m + 1) * pair_rows, :depth]
                    for m in (c_pairs, c_pairs + 1)
                    for ref in (near_ref, far_ref)
                    for x in range(ring)
                ],
                axis=0,
            )
            sums = []
            for b, step in ((2 * q, LANES - a_dev), (2 * q + 1, a_dev)):
                full = jnp.dot(amps, stack_ref[b], preferred_element_type=jnp.float32)
                full = full.reshape(blocks, 2, a_dev, LANES)
                mixed = jnp.where(odd, full[:, 1], full[:, 0]).reshape(blocks * a_dev, LANES)
                sums.append(mixed + pltpu.roll(mixed, step, 1))
            found = jnp.where(odd[0], sums[1], sums[0]).astype(out_ref.dtype)
            quarter, pair = own ^ (2 * q // some), q % (some // 2)
            column = pl.multiple_of((quarter * (some // 2) + pair) * LANES, LANES)
            for block in range(blocks):
                other_yh, other_core, x = block // (2 * ring), block // ring % 2, block % ring
                place = (lax.rem(yh + other_yh, 2) * ring + x) * 2 + lax.rem(core + other_core, 2)
                for h in range(2):
                    low = block * a_dev + h * (a_dev // 2)
                    out_ref[2 * place + h, :, pl.ds(column, LANES)] = found[low : low + a_dev // 2]


def in_vmem(count):
    return [pl.BlockSpec(memory_space=pltpu.VMEM)] * count


def ladder_partials(place, near, far, quarters, b_count, i_count, con_count):
    right = (len(quarters) * quarters[0].shape[0], quarters[0].shape[1])
    depth = (near.shape[1] // b_count - 2) * (right[0] // b_count)
    pairs = 2 * near.size * right[0]
    return pl.pallas_call(
        ladder_kernel,
        out_shape=jax.ShapeDtypeStruct(
            (con_count, i_count // con_count, b_count * LANES // 2), jnp.bfloat16
        ),
        in_specs=[pl.BlockSpec(memory_space=pltpu.SMEM)] + in_vmem(1 + len(quarters))
        + [pl.BlockSpec(memory_space=pl.ANY)],
        out_specs=pl.BlockSpec(memory_space=pltpu.VMEM),
        scratch_shapes=[
            pltpu.VMEM((b_count, depth, LANES), jnp.bfloat16),
            pltpu.VMEM(quarters[-1].shape, jnp.bfloat16),
            pltpu.SemaphoreType.DMA,
        ],
        compiler_params=pltpu.CompilerParams(vmem_limit_bytes=12 * 1024 * 1024),
        cost_estimate=pl.CostEstimate(
            flops=2 * pairs, bytes_accessed=4 * near.size, transcendentals=0
        ),
    )(place, near, far, *quarters)


def pack_kernel(rows_ref, amps_ref, other_ref, out_ref):
    count, cells = rows_ref.shape[0], amps_ref.shape[1] // 2
    for n in range(out_ref.shape[0]):
        out_ref[n, :count, :] = rows_ref[...]
    out_ref[:, count:, cells:] = jnp.zeros_like(out_ref[:, count:, cells:])
    for m, ref in enumerate((amps_ref, other_ref)):
        block = jnp.concatenate([ref[:, :cells], ref[:, cells:]], axis=0)
        for n in range(out_ref.shape[0]):
            first = count + m * block.shape[0]
            out_ref[n, first : first + block.shape[0], :cells] = block


def packed_copies(rows, amps, other, copies):
    count = rows.shape[0] + 4 * amps.shape[0]
    return pl.pallas_call(
        pack_kernel,
        out_shape=jax.ShapeDtypeStruct((copies, count, rows.shape[1]), rows.dtype),
        in_specs=in_vmem(3),
        out_specs=pl.BlockSpec(memory_space=pltpu.VMEM),
        compiler_params=pltpu.CompilerParams(vmem_limit_bytes=6 * 1024 * 1024),
        cost_estimate=pl.CostEstimate(
            flops=rows.size, bytes_accessed=16 * rows.size, transcendentals=0
        ),
    )(rows, amps, other)


def total_kernel(parts_ref, out_ref):
    total = parts_ref[0].astype(jnp.float32)
    for k in range(1, parts_ref.shape[0]):
        total = total + parts_ref[k].astype(jnp.float32)
    total = total.astype(out_ref.dtype)
    for o in range(out_ref.shape[0]):
        out_ref[o] = total


def totals(parts, copies):
    return pl.pallas_call(
        total_kernel,
        out_shape=jax.ShapeDtypeStruct((copies, *parts.shape[1:]), parts.dtype),
        in_specs=in_vmem(1),
        out_specs=pl.BlockSpec(memory_space=pltpu.VMEM),
        compiler_params=pltpu.CompilerParams(vmem_limit_bytes=4 * 1024 * 1024),
        cost_estimate=pl.CostEstimate(
            flops=parts.size, bytes_accessed=4 * parts.size, transcendentals=0
        ),
    )(parts)


def residual_kernel(ring, pairs_ref, swap_ref, every_ref, out_ref):
    slots, occ, width = out_ref.shape
    group = LANES // ring
    chunks = every_ref.shape[2] // LANES // 2
    lane_group = lax.broadcasted_iota(jnp.int32, (1, LANES), 1) // group

    def half_tile(a_tile, b_tile, c):
        holder = (a_tile // ring * ring + lax.rem(b_tile, ring)) * 2 + c
        first = b_tile // ring * (chunks * LANES)
        found = jnp.zeros((occ, LANES), jnp.float32)
        for m in range(chunks):
            block = every_ref[holder, :, pl.ds(pl.multiple_of(first + m * LANES, LANES), LANES)]
            block = block.astype(jnp.float32)
            shift = lax.rem((m + ring - lax.rem(a_tile, ring)) * group, LANES)
            found = jnp.where(lane_group == m, pltpu.roll(block, shift, 1), found)
        return found

    def tiles(role):
        return jnp.concatenate(
            [
                jnp.concatenate(
                    [half_tile(pairs_ref[s, role], pairs_ref[s, 1 - role], c) for c in range(2)],
                    axis=1,
                )
                for s in range(slots)
            ],
            axis=0,
        ).astype(jnp.bfloat16)

    def placed(rows, spot):
        column = lax.broadcasted_iota(jnp.int32, (width, width), 1)
        chosen = (column == spot).astype(jnp.float32).astype(jnp.bfloat16)
        return jnp.dot(rows, chosen, preferred_element_type=jnp.float32)

    lane = lax.broadcasted_iota(jnp.int32, (width, width), 0)
    core_b = lane // LANES
    core_a = lax.rem(lane // (group // 2) + core_b, 2)
    a = core_a * (TS // 2) + lax.rem(lane, TS // 2)
    b = core_b * (TS // 2) + lax.rem(lane, LANES) // group * 2 + lax.rem(lane // (TS // 2), 2)
    straight = placed(tiles(0), a * TS + b)
    row = lax.broadcasted_iota(jnp.int32, (slots * occ, slots * occ), 0)
    column = lax.broadcasted_iota(jnp.int32, (slots * occ, slots * occ), 1)
    source = row // occ * occ
    for i in range(occ):
        source = source + jnp.where(lax.rem(row, occ) == i, swap_ref[i], 0)
    chosen = (column == source).astype(jnp.float32).astype(jnp.bfloat16)
    swapped = jnp.dot(chosen, tiles(1), preferred_element_type=jnp.float32).astype(jnp.bfloat16)
    total = straight + placed(swapped, b * TS + a)
    for s in range(slots):
        out_ref[s] = total[s * occ : (s + 1) * occ]


def residual_tiles(pairs, swap, every, ring):
    slots, occ = pairs.shape[0], swap.shape[0]
    return pl.pallas_call(
        functools.partial(residual_kernel, ring),
        out_shape=jax.ShapeDtypeStruct((slots, occ, TS * TS), jnp.float32),
        in_specs=[pl.BlockSpec(memory_space=pltpu.SMEM)] * 2 + in_vmem(1),
        out_specs=pl.BlockSpec(memory_space=pltpu.VMEM),
        compiler_params=pltpu.CompilerParams(vmem_limit_bytes=8 * 1024 * 1024),
        cost_estimate=pl.CostEstimate(
            flops=100 * every.size, bytes_accessed=4 * every.size, transcendentals=0
        ),
    )(pairs, swap, every)


def on_device(chol, amplitudes, tile_pairs, partner, pair_swap):
    out_count = lax.axis_size(OUT)
    con_count = lax.axis_size(CONTRACT)
    ring = lax.axis_size("x")
    a_dev, c_dev, p_size = chol.shape
    i_count = amplitudes.shape[0] * out_count
    half = c_dev // 2

    other_amps = lax.ppermute(amplitudes, "yh", PAIR)
    rows = jnp.transpose(chol.reshape(a_dev, 2, half, p_size), (2, 1, 0, 3))
    packed = packed_copies(rows.reshape(-1, p_size), amplitudes, other_amps, ring)
    near = exchange(packed, "x")

    z, yl, yh = lax.axis_index("z"), lax.axis_index("yl"), lax.axis_index("yh")
    depth_z = lax.axis_size("z")
    window = chol.reshape(2, -1, p_size)
    piece = jnp.where(yl == 0, window[0], lax.ppermute(window[1], CONTRACT, [(0, 1)]))
    got = sum(lax.ppermute(piece, "z", [hop]) for hop in LONG)
    piece = jnp.where(z == 0, piece, got)
    got = lax.ppermute(piece, "z", MIDDLE)
    piece = jnp.where(functools.reduce(jnp.logical_or, [z == to for _, to in MIDDLE]), got, piece)
    reach = {}
    for to in range(depth_z):
        if to not in SENDERS:
            steps = [((to - at + depth_z // 2) % depth_z - depth_z // 2, at) for at in SENDERS]
            step, at = min(steps, key=lambda pair: abs(pair[0]))
            reach.setdefault(step, []).append((at, to))
    steps = sorted(reach, key=abs, reverse=True)
    got = lax.ppermute(piece, "z", reach[steps[0]])
    got = sum((lax.ppermute(piece, "z", reach[step]) for step in steps[1:]), got)
    sender = functools.reduce(jnp.logical_or, [z == at for at in SENDERS])
    piece = jnp.where(sender, piece, got)
    quarters = [piece] + [
        lax.ppermute(piece, ("yl", "yh"), [(at, at ^ q) for at in range(4)]) for q in (2, 1, 3)
    ]

    far = lax.ppermute(near, "core", PAIR)
    slot_count, occ_dev = tile_pairs.shape[0] // out_count, i_count // con_count
    first = lax.axis_index(OUT) * slot_count
    pairs = lax.dynamic_slice_in_dim(tile_pairs, first, slot_count, 0)
    first = lax.axis_index(CONTRACT) * occ_dev
    swap = lax.dynamic_slice_in_dim(pair_swap, first, occ_dev, 0) - first
    far, pairs, swap = lax.optimization_barrier((far, pairs, swap))
    place = jnp.stack([lax.axis_index("core"), yh, 2 * yh + yl])
    partial = ladder_partials(place, near, far, quarters, 2 * a_dev, i_count, con_count)
    every = exchange(totals(exchange(partial, CONTRACT), out_count), OUT)

    return residual_tiles(pairs, swap, every, ring)


def solution(mesh):
    torus = Mesh(mesh.devices.reshape(16, 2, 2, 4, 2), ("z", "yl", "yh", "x", "core"))
    in_specs = (P(OUT, CONTRACT, None), P(OUT, CONTRACT), P(), P(), P())
    out_specs = P(OUT, CONTRACT, None)

    return jax.shard_map(
        on_device, mesh=torus, in_specs=in_specs, out_specs=out_specs, check_vma=False
    )
```

```python
import functools

import jax
import jax.numpy as jnp
from jax import lax
from jax.experimental import pallas as pl
from jax.experimental.pallas import tpu as pltpu
from jax.sharding import Mesh
from jax.sharding import PartitionSpec as P

TS = 16
LANES = 128
CONTRACT = ("z", "yl")
OUT = ("yh", "x", "core")
PAIR = [(0, 1), (1, 0)]
LONG, MIDDLE = [(0, 3), (0, 13)], [(3, 6), (13, 10)]
SENDERS = (0, 3, 6, 10, 13)


def exchange(array, axes):
    return lax.all_to_all(array, axes, 0, 0, tiled=True)


def ladder_kernel(place_ref, near_ref, far_ref, *refs):
    *quarter_refs, out_ref, stack_ref = refs
    core, yh, own = place_ref[0], place_ref[1], place_ref[2]
    b_count, depth, _ = stack_ref.shape
    ring, pair_rows = near_ref.shape[0], b_count
    c_pairs = near_ref.shape[1] // pair_rows - 2
    a_dev = pair_rows // 2
    some = b_count // len(quarter_refs)
    d_count = quarter_refs[0].shape[0] // some
    together = len(quarter_refs)
    odd = lax.rem(lax.broadcasted_iota(jnp.int32, (1, 1, LANES), 2) // a_dev, 2) == 1
    blocks = 4 * ring
    for first in range(0, len(quarter_refs), together):
        for n in range(0, c_pairs, 2):
            left = jnp.concatenate(
                [
                    ref[x, m * pair_rows : (m + 1) * pair_rows, :]
                    for m in (n, n + 1)
                    for x in range(ring)
                    for ref in (near_ref, far_ref)
                ],
                axis=0,
            )
            right = jnp.concatenate([ref[...] for ref in quarter_refs[first : first + together]], axis=0)
            part = lax.dot_general(
                right, left, (((1,), (1,)), ((), ())), preferred_element_type=jnp.float32
            ).astype(jnp.bfloat16)
            part = part.reshape(together * some, d_count, 2 * LANES)
            for h in range(2):
                rows = (n + h) * d_count
                stack_ref[first * some : (first + together) * some, rows : rows + d_count, :] = part[
                    :, :, h * LANES : (h + 1) * LANES
                ]
        for q in range(first * some // 2, (first + together) * some // 2):
            amps = jnp.concatenate(
                [
                    ref[x, m * pair_rows : (m + 1) * pair_rows, :depth]
                    for m in (c_pairs, c_pairs + 1)
                    for ref in (near_ref, far_ref)
                    for x in range(ring)
                ],
                axis=0,
            )
            sums = []
            for b, step in ((2 * q, LANES - a_dev), (2 * q + 1, a_dev)):
                full = jnp.dot(amps, stack_ref[b], preferred_element_type=jnp.float32)
                full = full.reshape(blocks, 2, a_dev, LANES)
                mixed = jnp.where(odd, full[:, 1], full[:, 0]).reshape(blocks * a_dev, LANES)
                sums.append(mixed + pltpu.roll(mixed, step, 1))
            found = jnp.where(odd[0], sums[1], sums[0]).astype(out_ref.dtype)
            quarter, pair = own ^ (2 * q // some), q % (some // 2)
            column = pl.multiple_of((quarter * (some // 2) + pair) * LANES, LANES)
            for block in range(blocks):
                other_yh, other_core, x = block // (2 * ring), block // ring % 2, block % ring
                place = (lax.rem(yh + other_yh, 2) * ring + x) * 2 + lax.rem(core + other_core, 2)
                for h in range(2):
                    low = block * a_dev + h * (a_dev // 2)
                    out_ref[2 * place + h, :, pl.ds(column, LANES)] = found[low : low + a_dev // 2]


def in_vmem(count):
    return [pl.BlockSpec(memory_space=pltpu.VMEM)] * count


def ladder_partials(place, near, far, quarters, b_count, i_count, con_count):
    right = (len(quarters) * quarters[0].shape[0], quarters[0].shape[1])
    depth = (near.shape[1] // b_count - 2) * (right[0] // b_count)
    pairs = 2 * near.size * right[0]
    return pl.pallas_call(
        ladder_kernel,
        out_shape=jax.ShapeDtypeStruct(
            (con_count, i_count // con_count, b_count * LANES // 2), jnp.bfloat16
        ),
        in_specs=[pl.BlockSpec(memory_space=pltpu.SMEM)] + in_vmem(2 + len(quarters)),
        out_specs=pl.BlockSpec(memory_space=pltpu.VMEM),
        scratch_shapes=[
            pltpu.VMEM((b_count, depth, LANES), jnp.bfloat16),
        ],
        compiler_params=pltpu.CompilerParams(vmem_limit_bytes=12 * 1024 * 1024),
        cost_estimate=pl.CostEstimate(
            flops=2 * pairs, bytes_accessed=4 * near.size, transcendentals=0
        ),
    )(place, near, far, *quarters)


def pack_kernel(rows_ref, amps_ref, other_ref, out_ref):
    count, cells = rows_ref.shape[0], amps_ref.shape[1] // 2
    for n in range(out_ref.shape[0]):
        out_ref[n, :count, :] = rows_ref[...]
    out_ref[:, count:, cells:] = jnp.zeros_like(out_ref[:, count:, cells:])
    for m, ref in enumerate((amps_ref, other_ref)):
        block = jnp.concatenate([ref[:, :cells], ref[:, cells:]], axis=0)
        for n in range(out_ref.shape[0]):
            first = count + m * block.shape[0]
            out_ref[n, first : first + block.shape[0], :cells] = block


def packed_copies(rows, amps, other, copies):
    count = rows.shape[0] + 4 * amps.shape[0]
    return pl.pallas_call(
        pack_kernel,
        out_shape=jax.ShapeDtypeStruct((copies, count, rows.shape[1]), rows.dtype),
        in_specs=in_vmem(3),
        out_specs=pl.BlockSpec(memory_space=pltpu.VMEM),
        compiler_params=pltpu.CompilerParams(vmem_limit_bytes=6 * 1024 * 1024),
        cost_estimate=pl.CostEstimate(
            flops=rows.size, bytes_accessed=16 * rows.size, transcendentals=0
        ),
    )(rows, amps, other)


def total_kernel(parts_ref, out_ref):
    total = parts_ref[0].astype(jnp.float32)
    for k in range(1, parts_ref.shape[0]):
        total = total + parts_ref[k].astype(jnp.float32)
    total = total.astype(out_ref.dtype)
    for o in range(out_ref.shape[0]):
        out_ref[o] = total


def totals(parts, copies):
    return pl.pallas_call(
        total_kernel,
        out_shape=jax.ShapeDtypeStruct((copies, *parts.shape[1:]), parts.dtype),
        in_specs=in_vmem(1),
        out_specs=pl.BlockSpec(memory_space=pltpu.VMEM),
        compiler_params=pltpu.CompilerParams(vmem_limit_bytes=4 * 1024 * 1024),
        cost_estimate=pl.CostEstimate(
            flops=parts.size, bytes_accessed=4 * parts.size, transcendentals=0
        ),
    )(parts)


def residual_kernel(ring, pairs_ref, swap_ref, every_ref, out_ref):
    slots, occ, width = out_ref.shape
    group = LANES // ring
    chunks = every_ref.shape[2] // LANES // 2
    lane_group = lax.broadcasted_iota(jnp.int32, (1, LANES), 1) // group

    def half_tile(a_tile, b_tile, c):
        holder = (a_tile // ring * ring + lax.rem(b_tile, ring)) * 2 + c
        first = b_tile // ring * (chunks * LANES)
        found = jnp.zeros((occ, LANES), jnp.float32)
        for m in range(chunks):
            block = every_ref[holder, :, pl.ds(pl.multiple_of(first + m * LANES, LANES), LANES)]
            block = block.astype(jnp.float32)
            shift = lax.rem((m + ring - lax.rem(a_tile, ring)) * group, LANES)
            found = jnp.where(lane_group == m, pltpu.roll(block, shift, 1), found)
        return found

    def tiles(role):
        return jnp.concatenate(
            [
                jnp.concatenate(
                    [half_tile(pairs_ref[s, role], pairs_ref[s, 1 - role], c) for c in range(2)],
                    axis=1,
                )
                for s in range(slots)
            ],
            axis=0,
        ).astype(jnp.bfloat16)

    def placed(rows, spot):
        column = lax.broadcasted_iota(jnp.int32, (width, width), 1)
        chosen = (column == spot).astype(jnp.float32).astype(jnp.bfloat16)
        return jnp.dot(rows, chosen, preferred_element_type=jnp.float32)

    lane = lax.broadcasted_iota(jnp.int32, (width, width), 0)
    core_b = lane // LANES
    core_a = lax.rem(lane // (group // 2) + core_b, 2)
    a = core_a * (TS // 2) + lax.rem(lane, TS // 2)
    b = core_b * (TS // 2) + lax.rem(lane, LANES) // group * 2 + lax.rem(lane // (TS // 2), 2)
    straight = placed(tiles(0), a * TS + b)
    row = lax.broadcasted_iota(jnp.int32, (slots * occ, slots * occ), 0)
    column = lax.broadcasted_iota(jnp.int32, (slots * occ, slots * occ), 1)
    source = row // occ * occ
    for i in range(occ):
        source = source + jnp.where(lax.rem(row, occ) == i, swap_ref[i], 0)
    chosen = (column == source).astype(jnp.float32).astype(jnp.bfloat16)
    swapped = jnp.dot(chosen, tiles(1), preferred_element_type=jnp.float32).astype(jnp.bfloat16)
    total = straight + placed(swapped, b * TS + a)
    for s in range(slots):
        out_ref[s] = total[s * occ : (s + 1) * occ]


def residual_tiles(pairs, swap, every, ring):
    slots, occ = pairs.shape[0], swap.shape[0]
    return pl.pallas_call(
        functools.partial(residual_kernel, ring),
        out_shape=jax.ShapeDtypeStruct((slots, occ, TS * TS), jnp.float32),
        in_specs=[pl.BlockSpec(memory_space=pltpu.SMEM)] * 2 + in_vmem(1),
        out_specs=pl.BlockSpec(memory_space=pltpu.VMEM),
        compiler_params=pltpu.CompilerParams(vmem_limit_bytes=8 * 1024 * 1024),
        cost_estimate=pl.CostEstimate(
            flops=100 * every.size, bytes_accessed=4 * every.size, transcendentals=0
        ),
    )(pairs, swap, every)


def on_device(chol, amplitudes, tile_pairs, partner, pair_swap):
    out_count = lax.axis_size(OUT)
    con_count = lax.axis_size(CONTRACT)
    ring = lax.axis_size("x")
    a_dev, c_dev, p_size = chol.shape
    i_count = amplitudes.shape[0] * out_count
    half = c_dev // 2

    other_amps = lax.ppermute(amplitudes, "yh", PAIR)
    rows = jnp.transpose(chol.reshape(a_dev, 2, half, p_size), (2, 1, 0, 3))
    packed = packed_copies(rows.reshape(-1, p_size), amplitudes, other_amps, ring)
    near = exchange(packed, "x")

    z, yl, yh = lax.axis_index("z"), lax.axis_index("yl"), lax.axis_index("yh")
    depth_z = lax.axis_size("z")
    window = chol.reshape(2, -1, p_size)
    piece = jnp.where(yl == 0, window[0], lax.ppermute(window[1], CONTRACT, [(0, 1)]))
    got = sum(lax.ppermute(piece, "z", [hop]) for hop in LONG)
    piece = jnp.where(z == 0, piece, got)
    got = lax.ppermute(piece, "z", MIDDLE)
    piece = jnp.where(functools.reduce(jnp.logical_or, [z == to for _, to in MIDDLE]), got, piece)
    reach = {}
    for to in range(depth_z):
        if to not in SENDERS:
            steps = [((to - at + depth_z // 2) % depth_z - depth_z // 2, at) for at in SENDERS]
            step, at = min(steps, key=lambda pair: abs(pair[0]))
            reach.setdefault(step, []).append((at, to))
    steps = sorted(reach, key=abs, reverse=True)
    got = lax.ppermute(piece, "z", reach[steps[0]])
    got = sum((lax.ppermute(piece, "z", reach[step]) for step in steps[1:]), got)
    sender = functools.reduce(jnp.logical_or, [z == at for at in SENDERS])
    piece = jnp.where(sender, piece, got)
    quarters = [piece] + [
        lax.ppermute(piece, ("yl", "yh"), [(at, at ^ q) for at in range(4)]) for q in (2, 1)
    ]
    quarters.append(lax.ppermute(piece, ("yl", "yh"), [(at, at ^ 3) for at in range(4)]))

    far = lax.ppermute(near, "core", PAIR)
    slot_count, occ_dev = tile_pairs.shape[0] // out_count, i_count // con_count
    first = lax.axis_index(OUT) * slot_count
    pairs = lax.dynamic_slice_in_dim(tile_pairs, first, slot_count, 0)
    first = lax.axis_index(CONTRACT) * occ_dev
    swap = lax.dynamic_slice_in_dim(pair_swap, first, occ_dev, 0) - first
    far, pairs, swap = lax.optimization_barrier((far, pairs, swap))
    place = jnp.stack([lax.axis_index("core"), yh, 2 * yh + yl])
    partial = ladder_partials(place, near, far, quarters, 2 * a_dev, i_count, con_count)
    every = exchange(totals(exchange(partial, CONTRACT), out_count), OUT)

    return residual_tiles(pairs, swap, every, ring)


def solution(mesh):
    torus = Mesh(mesh.devices.reshape(16, 2, 2, 4, 2), ("z", "yl", "yh", "x", "core"))
    in_specs = (P(OUT, CONTRACT, None), P(OUT, CONTRACT), P(), P(), P())
    out_specs = P(OUT, CONTRACT, None)

    return jax.shard_map(
        on_device, mesh=torus, in_specs=in_specs, out_specs=out_specs, check_vma=False
    )
```
